256 devices in a mesh: row: 16 (over x, y), col: 16 (over z, core).
Axes of the slice: x: 4, y: 4, z: 8, core: 2. Of those that a mesh axis runs over, the one named last changes fastest.
Arguments:
- tiles: bfloat16 [16, 16, 128, 128, 128], P('row', 'col'), may hold values from 0 to 0.31
- block_rows: int32 [16, 16, 128], P('row', 'col'), may hold values from 0 to 255, as said below
- block_cols: int32 [16, 16, 128], P('row', 'col'), may hold values from 0 to 255
- counts: int32 [16, 16], P('row', 'col'), may hold values from 1 to 128, as said below
- seeds: int32 [8, 524288], P(None, ('col', 'row')), may hold values from 1 to 999
Outputs:
- vectors_out: float32 [8, 524288], P(None, ('col', 'row'))
- deltas: float32 [4, 8], replicated
The draws below stay inside these ranges and needn't reach their ends.
Inputs may be any that keep to these rules, and one draw needn't show every extreme that they name: `counts`: each entry is 1, a half, a quarter or an eighth of 128 (at least 1); some device is full in every draw. On each device, among the values of block_rows (over all 128 slots) that share one quotient by 16, at most 4 are distinct; on a device whose count is 128, some quotient has exactly 4 distinct values among its tiles.
All inputs are finite; a program needn't handle non-finite values.
Results may differ from the reference program's by a relative error of at most 0.00061.
Values may be sent and summed in bfloat16 or wider, within the bound.
A program may use at most 64 MiB of HBM per device.

```python
import jax
import jax.numpy as jnp
from jax import lax

K = 8
BLOCK = 128
ITERS = 4
PIECE_DEV = 2048
TILES_DEV = 128
NODES = 524288
ROW_BLOCKS = 256
COL_BLOCKS = 256
ROW_CAP = 4
N_ROW = 16
N_COL = 16


def draw_counts(key, part):
    level_key = jax.random.fold_in(key, 11)
    spot_key = jax.random.fold_in(key, 23)
    levels = jax.random.randint(level_key, (N_ROW * N_COL,), 0, 4)
    divided = TILES_DEV // jnp.power(2, levels).astype(jnp.int32)
    divided = jnp.maximum(divided, 1).astype(jnp.int32)
    chosen = jax.random.randint(spot_key, (), 0, N_ROW * N_COL)
    divided = divided.at[chosen].set(TILES_DEV)
    return divided.reshape(N_ROW, N_COL).astype(jnp.int32)


def distinct_order(key, rows, length):
    scores = jax.random.randint(key, (rows, length), 0, 1 << 20) * length + jnp.arange(length, dtype=jnp.int32)[None, :]
    return jnp.argsort(scores, axis=1).astype(jnp.int32)


def draw_block_rows(key, part):
    piece_blocks = PIECE_DEV // BLOCK
    devices_all = N_ROW * N_COL
    allowed_total = N_ROW * ROW_CAP
    offsets = distinct_order(jax.random.fold_in(key, 31), devices_all * N_ROW, piece_blocks)[:, :ROW_CAP]
    offsets = offsets.reshape(devices_all, N_ROW, ROW_CAP)
    owners = jnp.arange(N_ROW, dtype=jnp.int32)[None, :, None] * piece_blocks
    allowed = (owners + offsets).reshape(devices_all, allowed_total).astype(jnp.int32)
    ranks = distinct_order(jax.random.fold_in(key, 37), devices_all, TILES_DEV)
    picks = jax.random.randint(jax.random.fold_in(key, 41), (devices_all, TILES_DEV), 0, allowed_total)
    index = jnp.where(ranks < allowed_total, ranks, picks).astype(jnp.int32)
    chosen = jnp.take_along_axis(allowed, index, axis=1)
    return chosen.reshape(N_ROW, N_COL, TILES_DEV).astype(jnp.int32)


def row_classes(key):
    return jax.random.randint(jax.random.fold_in(key, 53), (NODES // BLOCK,), 0, 2).astype(jnp.int32)


def draw_tiles(key, part):
    mask_key = jax.random.fold_in(key, 5)
    weight_key = jax.random.fold_in(key, 7)
    shape = (N_ROW, N_COL, TILES_DEV, BLOCK, BLOCK)
    density = min(0.5, 16.0 * PIECE_DEV / (BLOCK * BLOCK * TILES_DEV))
    kept = jax.random.uniform(mask_key, shape, dtype=jnp.float32) < density
    local_rows = draw_block_rows(key, part)
    segment_base = jnp.arange(N_COL, dtype=jnp.int32)[None, :, None] * ROW_BLOCKS
    classes = row_classes(key)[(local_rows + segment_base).astype(jnp.int32)]
    heavy_rows = (classes == 1)[:, :, :, None, None]
    spread = jax.random.uniform(weight_key, shape, dtype=jnp.float32)
    light_weight = jnp.exp(jnp.log(0.01) + spread * (jnp.log(0.04) - jnp.log(0.01)))
    heavy_weight = jnp.exp(jnp.log(0.12) + spread * (jnp.log(0.3) - jnp.log(0.12)))
    weights = jnp.where(heavy_rows, heavy_weight, light_weight)
    return jnp.where(kept, weights, 0.0).astype(jnp.bfloat16)


def draw_seeds(key, part):
    node_index = jnp.arange(NODES, dtype=jnp.int32)
    node_block = (node_index // BLOCK).astype(jnp.int32)
    node_class = row_classes(key)[node_block]
    threshold = jax.random.randint(jax.random.fold_in(key, 61), (K, 1), 4, 9)
    rolls = jax.random.randint(jax.random.fold_in(key, 67), (K, NODES // BLOCK), 0, 8)
    node_rolls = rolls[:, node_block]
    raised = jnp.where(node_class[None, :] == 0, node_rolls < threshold, node_rolls < 1)
    high_value = jax.random.randint(jax.random.fold_in(key, 71), (K, NODES), 500, 1000)
    low_value = jax.random.randint(jax.random.fold_in(key, 73), (K, NODES), 1, 40)
    return jnp.where(raised, high_value, low_value).astype(jnp.int32)


def set_ends(result, key, least, top_value):
    longest = result.shape.index(max(result.shape))
    spots = []
    for shift in (0, 1):
        where = [jax.random.randint(jax.random.fold_in(key, axis), (), 0, length) for axis, length in enumerate(result.shape)]
        where[longest] = (where[longest] + shift) % result.shape[longest]
        spots.append(tuple(where))
    return result.at[spots[0]].set(least).at[spots[1]].set(top_value)


def setup_inputs(seed: int = 0) -> dict:
    arg_keys = jax.random.split(jax.random.key(seed), 6)
    tiles = draw_tiles(jax.random.fold_in(arg_keys[5], 71), 0)
    block_rows = draw_block_rows(jax.random.fold_in(arg_keys[5], 71), 0)
    block_cols = set_ends(jax.random.randint(arg_keys[2], (N_ROW, N_COL, TILES_DEV), 0, COL_BLOCKS), jax.random.fold_in(arg_keys[2], 1), 0, COL_BLOCKS - 1).astype(jnp.int32)
    counts = draw_counts(jax.random.fold_in(arg_keys[5], 71), 0)
    seeds = draw_seeds(jax.random.fold_in(arg_keys[5], 71), 0)
    return {"tiles": tiles, "block_rows": block_rows, "block_cols": block_cols, "counts": counts, "seeds": seeds}


def reference(tiles, block_rows, block_cols, counts, seeds):
    piece_blocks = PIECE_DEV // BLOCK
    row_span = N_ROW * piece_blocks
    total_nodes = PIECE_DEV * N_ROW * N_COL
    devices_all = N_ROW * N_COL
    all_blocks = total_nodes // BLOCK
    flat_tiles = tiles.reshape(devices_all, TILES_DEV, BLOCK, BLOCK)
    flat_rows = block_rows.reshape(devices_all, TILES_DEV).astype(jnp.int32)
    flat_cols = block_cols.reshape(devices_all, TILES_DEV).astype(jnp.int32)
    flat_counts = counts.reshape(devices_all).astype(jnp.int32)
    positions = jnp.arange(devices_all, dtype=jnp.int32)
    row_index = positions // N_COL
    col_index = positions % N_COL
    tile_index = jnp.arange(TILES_DEV, dtype=jnp.int32)
    global_rows = (col_index[:, None] * row_span + flat_rows).astype(jnp.int32)
    global_cols = (((flat_cols // piece_blocks) * N_ROW + row_index[:, None]) * piece_blocks + flat_cols % piece_blocks).astype(jnp.int32)
    live_mask = (tile_index[None, :] < flat_counts[:, None]).astype(jnp.float32)

    def add_degree(running, entry_data):
        panel_here, rows_here, live_here = entry_data
        row_total = jnp.sum(panel_here.astype(jnp.float32), axis=2) * live_here[:, None]
        return running.at[rows_here].add(row_total), None

    degree = lax.scan(add_degree, jnp.zeros((all_blocks, BLOCK), jnp.float32), (flat_tiles, global_rows, live_mask))[0]
    divisor = 1.0 + degree[:, None, :]
    seed_float = seeds.astype(jnp.float32)
    start_vec = total_nodes * seed_float / jnp.sum(seed_float, axis=1, keepdims=True)
    current = start_vec.reshape(K, all_blocks, BLOCK).transpose(1, 0, 2)
    deltas = []
    for iteration in range(ITERS):
        half_vec = lax.optimization_barrier(current.astype(jnp.bfloat16))

        def add_product(running, entry_data, source=half_vec):
            panel_here, rows_here, cols_here, live_here = entry_data
            taken_rows = source[cols_here].astype(jnp.float32)
            product = jnp.einsum("tkc,trc->tkr", taken_rows, panel_here.astype(jnp.float32), precision=lax.Precision.HIGHEST)
            return running.at[rows_here].add(product * live_here[:, None, None]), None

        image = lax.scan(add_product, jnp.zeros((all_blocks, K, BLOCK), jnp.float32), (flat_tiles, global_rows, global_cols, live_mask))[0]
        raw_next = (image + current) / divisor
        totals = jnp.sum(raw_next, axis=(0, 2))
        updated = total_nodes * raw_next / totals[None, :, None]
        deltas.append(jnp.max(jnp.abs(updated - current), axis=(0, 2)))
        current = updated
    return current.transpose(1, 0, 2).reshape(K, total_nodes), jnp.stack(deltas)
```

```python
import functools

import jax
import jax.numpy as jnp
from jax import lax
from jax.experimental import pallas as pl
from jax.experimental.pallas import tpu as pltpu
from jax.sharding import PartitionSpec as P

BLOCK = 128
ITERS = 4
ROW_CAP = 4
K = 8
UNROLL = 16
DEAD = 1024
NT = (((1,), (1,)), ((), ()))
F32 = jnp.float32


def within(index, most):
    return jnp.minimum(jnp.maximum(index, 0), most)


def ring(delta, size):
    return min(delta % size, -delta % size)


def kernel(
    nx, ny, nz, pb, nodes,
    tiles_ref, rows_ref, cols_ref, counts_ref, seeds_ref,
    out_ref, deltas_ref,
    a_buf, g_even, g_odd, y_buf, p_buf, inc_even, inc_odd, v_buf, raw_buf, deg_buf,
    tab_v, tab_s, rank_v, ctab_v, ctab_s, ar_a, ar_b, st_a, st_b,
    a_sem, tab_sem, gr_sem, gs_sem, er_sem, es_sem, cr_sem, cs_sem, ra_sem, sa_sem, rb_sem, sb_sem,
):
    n_row, n_col = nx * ny, nz * 2
    g_buf, inc_buf = (g_even, g_odd), (inc_even, inc_odd)
    tile_total = a_buf.shape[0]
    slots = n_row * ROW_CAP
    i = lax.axis_index("row")
    j = lax.axis_index("col")
    px, py = i // ny, i % ny
    z, c = j // 2, j % 2
    other = z * 2 + (1 - c)

    row_offsets = sorted(
        [(dx, dy) for dx in range(nx) for dy in range(ny) if (dx, dy) != (0, 0)],
        key=lambda d: -(ring(d[0], nx) + ring(d[1], ny)),
    )
    z_offsets = sorted(range(1, nz), key=lambda d: -ring(d, nz))

    def row_peer(d):
        return lax.rem(px + d[0], nx) * ny + lax.rem(py + d[1], ny)

    def col_of(dz):
        return lax.rem(z + dz, nz) * 2 + c

    load = pltpu.make_async_copy(tiles_ref.at[0, 0], a_buf, a_sem)
    load.start()

    barrier = pltpu.get_barrier_semaphore()
    for d in row_offsets:
        pl.semaphore_signal(barrier, inc=1, device_id={"row": row_peer(d)})
    for o in range(1, n_col):
        pl.semaphore_signal(barrier, inc=1, device_id={"col": lax.rem(j + o, n_col)})

    I32 = jnp.int32
    sub = lax.broadcasted_iota(I32, (tile_total, 128), 0)
    lane = lax.broadcasted_iota(I32, (tile_total, 128), 1)
    count = counts_ref[0, 0]
    lane_row = lax.broadcasted_iota(I32, (1, 128), 1)
    key_r = jnp.where(lane_row < count, rows_ref[0], DEAD)
    key_rr = jnp.broadcast_to(key_r, (tile_total, 128))
    cols_rr = jnp.broadcast_to(cols_ref[0], (tile_total, 128))

    def lanes(value):
        return jnp.sum(value, axis=1, keepdims=True)

    def subs(value):
        return jnp.sum(value, axis=0, keepdims=True)

    def pick_if(mask, value):
        return jnp.where(mask, value, 0)

    key_c = lanes(pick_if(sub == lane, key_rr))
    cols_c = lanes(pick_if(sub == lane, cols_rr))
    key_cc = jnp.broadcast_to(key_c, (tile_total, 128))
    same = key_rr == key_cc
    before = lanes(pick_if(same & (lane < sub), 1))
    pos_c = before + lanes(pick_if(key_rr < key_cc, 1))
    last_c = lanes(pick_if(key_rr <= key_cc, 1)) - 1
    first_c = pick_if((before == 0) & (key_c < DEAD), 1)
    before_r = subs(pick_if(same & (sub < lane), 1))
    first_r = pick_if((before_r == 0) & (key_r < DEAD), 1)
    shift = pb.bit_length() - 1
    owner_c = key_c >> shift
    owner_r = key_r >> shift
    rank_c = lanes(
        pick_if((owner_r == owner_c) & (key_rr < key_cc), jnp.broadcast_to(first_r, sub.shape))
    )
    order = pos_c == lane
    perm_r = subs(pick_if(order, sub))
    cols_sorted = subs(pick_if(order, cols_c))
    keep_r = subs(pick_if(order, 1 - first_c))
    slot_c = owner_c * ROW_CAP + rank_c
    chosen = slot_c == lane
    end_r = subs(pick_if(chosen, first_c * last_c)) + (1 - subs(pick_if(chosen, first_c))) * tile_total
    tab_v[0] = perm_r
    tab_v[1] = cols_sorted
    tab_v[2] = keep_r
    tab_v[3] = end_r
    halves = rank_v.shape[0]
    per_half = 128 // pb
    for h in range(halves):
        found = subs(pick_if(key_c == lane + 128 * h, first_c * (rank_c + 1)))
        rank_v[h] = jnp.where(found > 0, found - 1 + i * ROW_CAP, slots)
    table = pltpu.make_async_copy(tab_v, tab_s, tab_sem)
    table.start()

    y_buf[tile_total] = jnp.zeros((K, BLOCK), F32)
    for par in range(2):
        inc_buf[par][slots] = jnp.zeros((K, BLOCK), F32)
    g_odd[...] = jnp.ones(g_odd.shape, jnp.bfloat16)

    seed_sum = jnp.zeros((K, BLOCK), F32)
    for b in range(pb):
        seed_sum += seeds_ref[:, b * BLOCK : (b + 1) * BLOCK].astype(F32)

    table.wait()
    load.wait()

    def products(par):
        def step(at, acc):
            for u in range(UNROLL):
                t = at * UNROLL + u
                x = g_buf[par][within(tab_s[1, 0, t], n_col * pb - 1)]
                a = a_buf[within(tab_s[0, 0, t], tile_total - 1)]
                y = lax.dot_general(x, a, NT, preferred_element_type=F32)
                acc = acc * tab_s[2, 0, t].astype(F32) + y
                y_buf[t] = acc
            return acc

        lax.fori_loop(0, tile_total // UNROLL, step, jnp.zeros((K, BLOCK), F32))

        def pick(at, carry):
            for u in range(8):
                q = at * 8 + u
                p_buf[par, q] = y_buf[within(tab_s[3, 0, q], tile_total)]
            return carry

        lax.fori_loop(0, slots // 8, pick, 0)

    def exchange_copy(par, d):
        o = row_peer(d)
        index = d[0] * ny + d[1]
        return pltpu.make_async_remote_copy(
            src_ref=p_buf.at[par, pl.ds(o * ROW_CAP, ROW_CAP)],
            dst_ref=inc_buf[par].at[pl.ds(i * ROW_CAP, ROW_CAP)],
            send_sem=es_sem.at[par, index],
            recv_sem=er_sem.at[par, index],
            device_id={"row": o},
        )

    def exchange_start(par):
        for d in row_offsets:
            exchange_copy(par, d).start()
        inc_buf[par][pl.ds(i * ROW_CAP, ROW_CAP)] = p_buf[par, pl.ds(i * ROW_CAP, ROW_CAP)]

    def exchange_wait(par):
        for d in reversed(row_offsets):
            exchange_copy(par, d).wait_recv()

    def exchange_done(par):
        for d in row_offsets:
            exchange_copy(par, d).wait_send()

    def rank_copy(d):
        o = row_peer(d)
        index = d[0] * ny + d[1]
        return pltpu.make_async_remote_copy(
            src_ref=rank_v.at[o // per_half],
            dst_ref=ctab_v.at[i],
            send_sem=cs_sem.at[index],
            recv_sem=cr_sem.at[index],
            device_id={"row": o},
        )

    def gather_copy(par, source, dest, sem):
        piece = g_buf[par].at[pl.ds(source * pb, pb)]
        return pltpu.make_async_remote_copy(
            src_ref=piece,
            dst_ref=piece,
            send_sem=gs_sem.at[par, sem],
            recv_sem=gr_sem.at[par, source],
            device_id={"col": dest},
        )

    def gather_start(par):
        for dz in z_offsets:
            gather_copy(par, j, col_of(dz), dz).start()
        gather_copy(par, j, other, 0).start()

    def gather_wait(par):
        for dz in reversed(z_offsets):
            source = col_of(dz)
            gather_copy(par, source, other, nz + dz).wait_recv()
            gather_copy(par, source, other, nz + dz).start()
        for dz in [0] + z_offsets[::-1]:
            source = lax.rem(z + dz, nz) * 2 + (1 - c)
            gather_copy(par, source, other, dz).wait_recv()

    def gather_done(par):
        for sem in range(2 * nz):
            if sem != nz:
                gather_copy(par, j, other, sem).wait_send()

    def ar_row(n, d):
        index = d[0] * ny + d[1]
        return pltpu.make_async_remote_copy(
            src_ref=st_a.at[n], dst_ref=ar_a.at[n, i],
            send_sem=sa_sem.at[n, index], recv_sem=ra_sem.at[n, index],
            device_id={"row": row_peer(d)},
        )

    def ar_col(n, o):
        return pltpu.make_async_remote_copy(
            src_ref=st_b.at[n], dst_ref=ar_b.at[n, j],
            send_sem=sb_sem.at[n, o], recv_sem=rb_sem.at[n, o],
            device_id={"col": lax.rem(j + o, n_col)},
        )

    def ar_start(n, value):
        st_a[n] = value
        ar_a[n, i] = value
        for d in row_offsets:
            ar_row(n, d).start()

    def ar_middle(n, op):
        for d in reversed(row_offsets):
            ar_row(n, d).wait_recv()
        value = functools.reduce(op, [ar_a[n, s] for s in range(n_row)])
        st_b[n] = value
        ar_b[n, j] = value
        for o in range(1, n_col):
            ar_col(n, o).start()

    def ar_end(n, op):
        for o in range(1, n_col):
            ar_col(n, o).wait_recv()
        value = functools.reduce(op, [ar_b[n, s] for s in range(n_col)])
        for d in row_offsets:
            ar_row(n, d).wait_send()
        for o in range(1, n_col):
            ar_col(n, o).wait_send()
        return value

    def received(par, b):
        at = lax.rem(i, per_half) * pb + b
        parts = [inc_buf[par][within(ctab_s[s, 0, at], slots)] for s in range(n_row)]
        while len(parts) > 1:
            parts = [sum(parts[k : k + 2]) for k in range(0, len(parts), 2)]
        return parts[0]

    def scale_of(total):
        return nodes / jnp.broadcast_to(jnp.sum(total, axis=1, keepdims=True), (K, BLOCK))

    pl.semaphore_wait(barrier, n_row + n_col - 2)

    ar_start(0, seed_sum)
    for d in row_offsets:
        rank_copy(d).start()
    ctab_v[i] = rank_v[i // per_half]
    products(1)
    exchange_start(1)
    ar_middle(0, jnp.add)
    seed_scale = nodes / jnp.broadcast_to(
        jnp.sum(ar_end(0, jnp.add), axis=1, keepdims=True), (K, BLOCK)
    )
    for b in range(pb):
        v = seeds_ref[:, b * BLOCK : (b + 1) * BLOCK].astype(F32) * seed_scale
        v_buf[b] = v
        g_even[j * pb + b] = v.astype(jnp.bfloat16)
    gather_start(0)

    for d in reversed(row_offsets):
        rank_copy(d).wait_recv()
    ctable = pltpu.make_async_copy(ctab_v, ctab_s, tab_sem)
    ctable.start()
    ctable.wait()
    exchange_wait(1)

    def degrees(b, carry):
        deg_buf[b] = received(1, b) + 1.0
        return carry

    lax.fori_loop(0, pb, degrees, 0)
    exchange_done(1)
    for d in row_offsets:
        rank_copy(d).wait_send()

    changes = []
    for it in range(ITERS):
        par = it % 2
        gather_wait(par)
        products(par)
        exchange_start(par)
        gather_done(par)
        exchange_wait(par)

        def advance(b, acc):
            raw = (received(par, b) + v_buf[b]) / deg_buf[b]
            raw_buf[b] = raw
            return acc + raw

        total = lax.fori_loop(0, pb, advance, jnp.zeros((K, BLOCK), F32))
        ar_start(it + 1, total)
        ar_middle(it + 1, jnp.add)
        factor = scale_of(ar_end(it + 1, jnp.add))
        change = jnp.zeros((K, BLOCK), F32)
        for b in range(pb):
            v = raw_buf[b] * factor
            change = jnp.maximum(change, jnp.abs(v - v_buf[b]))
            if it < ITERS - 1:
                v_buf[b] = v
                g_buf[1 - par][j * pb + b] = v.astype(jnp.bfloat16)
            else:
                out_ref[:, b * BLOCK : (b + 1) * BLOCK] = v
        if it < ITERS - 1:
            gather_start(1 - par)
        exchange_done(par)
        changes.append(jnp.max(change, axis=1, keepdims=True))

    sub8 = lax.broadcasted_iota(jnp.int32, (K, BLOCK), 0)
    lane8 = lax.broadcasted_iota(jnp.int32, (K, BLOCK), 1)
    packed = jnp.zeros((K, BLOCK), F32)
    for it in range(ITERS):
        as_row = jnp.sum(jnp.where(sub8 == lane8, changes[it], 0.0), axis=0, keepdims=True)
        packed = jnp.where(sub8 == it, as_row, packed)
    last = ITERS + 1
    ar_start(last, packed)
    ar_middle(last, jnp.maximum)
    most = ar_end(last, jnp.maximum)
    deltas_ref[...] = most[0:ITERS, 0:K]


def solution(mesh, shape=(4, 4, 8)):
    nx, ny, nz = shape

    def on_device(tiles, block_rows, block_cols, counts, seeds):
        n_row, n_col = nx * ny, nz * 2
        tile_total = tiles.shape[2]
        piece = seeds.shape[1]
        pb = piece // BLOCK
        slots = n_row * ROW_CAP
        halves = max(1, n_row * pb // 128)
        nodes = float(piece * n_row * n_col)
        dma = pltpu.SemaphoreType.DMA
        reductions = ITERS + 2
        body = functools.partial(kernel, nx, ny, nz, pb, nodes)
        vmem = pl.BlockSpec(memory_space=pltpu.VMEM)
        return pl.pallas_call(
            body,
            out_shape=(
                jax.ShapeDtypeStruct((K, piece), F32),
                jax.ShapeDtypeStruct((ITERS, K), F32),
            ),
            in_specs=[
                pl.BlockSpec(memory_space=pl.ANY), vmem, vmem,
                pl.BlockSpec(memory_space=pltpu.SMEM), vmem,
            ],
            out_specs=(vmem, vmem),
            scratch_shapes=[
                pltpu.VMEM((tile_total, BLOCK, BLOCK), jnp.bfloat16),
                pltpu.VMEM((n_col * pb, K, BLOCK), jnp.bfloat16),
                pltpu.VMEM((n_col * pb, K, BLOCK), jnp.bfloat16),
                pltpu.VMEM((tile_total + 1, K, BLOCK), F32),
                pltpu.VMEM((2, slots, K, BLOCK), F32),
                pltpu.VMEM((slots + 1, K, BLOCK), F32),
                pltpu.VMEM((slots + 1, K, BLOCK), F32),
                pltpu.VMEM((pb, K, BLOCK), F32),
                pltpu.VMEM((pb, K, BLOCK), F32),
                pltpu.VMEM((pb, K, BLOCK), F32),
                pltpu.VMEM((4, 1, 128), jnp.int32),
                pltpu.SMEM((4, 1, 128), jnp.int32),
                pltpu.VMEM((halves, 1, 128), jnp.int32),
                pltpu.VMEM((n_row, 1, 128), jnp.int32),
                pltpu.SMEM((n_row, 1, 128), jnp.int32),
                pltpu.VMEM((reductions, n_row, K, BLOCK), F32),
                pltpu.VMEM((reductions, n_col, K, BLOCK), F32),
                pltpu.VMEM((reductions, K, BLOCK), F32),
                pltpu.VMEM((reductions, K, BLOCK), F32),
                dma, dma,
                dma((2, n_col)), dma((2, 2 * nz)),
                dma((2, n_row)), dma((2, n_row)),
                dma((n_row,)), dma((n_row,)),
                dma((reductions, n_row)), dma((reductions, n_row)),
                dma((reductions, n_col)), dma((reductions, n_col)),
            ],
            compiler_params=pltpu.CompilerParams(collective_id=0, has_side_effects=True),
        )(tiles, block_rows[0], block_cols[0], counts, seeds)

    return jax.shard_map(
        on_device,
        mesh=mesh,
        in_specs=(
            P("row", "col", None, None, None),
            P("row", "col", None),
            P("row", "col", None),
            P("row", "col"),
            P(None, ("col", "row")),
        ),
        out_specs=(P(None, ("col", "row")), P()),
        check_vma=False,
    )
```

```python
import functools

import jax
import jax.numpy as jnp
from jax import lax
from jax.experimental import pallas as pl
from jax.experimental.pallas import tpu as pltpu
from jax.sharding import PartitionSpec as P

BLOCK = 128
ITERS = 4
ROW_CAP = 4
K = 8
UNROLL = 64
DEAD = 1024
F32 = jnp.float32
BF16 = jnp.bfloat16
I32 = jnp.int32


def within(index, most):
    return jnp.minimum(jnp.maximum(index, 0), most)


def ring(delta, size):
    return min(delta % size, -delta % size)


def split(value):
    high = value.astype(BF16)
    rest = value - high.astype(F32)
    middle = rest.astype(BF16)
    low = (rest - middle.astype(F32)).astype(BF16)
    return high, middle, low


def kernel(
    nx, ny, nz, pb, nodes,
    tiles_ref, rows_ref, cols_ref, counts_ref, seeds_ref,
    out_ref, deltas_ref,
    a_buf, t_buf, g_even, g_odd, s_all, y_buf, p_buf, inc_even, inc_odd, v_buf, raw_buf, w_buf,
    w_row, w_all, ut_buf, u_send, u_in, u_buf,
    tab_v, tab_s, rank_v, ctab_v, ctab_s, ar_a, ar_b, st_a, st_b,
    a_sem, tab_sem, gr_sem, gs_sem, er_sem, es_sem, cr_sem, cs_sem, ra_sem, sa_sem, rb_sem, sb_sem,
    wr_sem, ws_sem, ur_sem, us_sem,
):
    n_row, n_col = nx * ny, nz * 2
    g_buf, inc_buf = (g_even, g_odd, s_all), (inc_even, inc_odd)
    tile_total = a_buf.shape[0]
    slots = n_row * ROW_CAP
    row_blocks, col_blocks = n_row * pb, n_col * pb
    i = lax.axis_index("row")
    j = lax.axis_index("col")
    px, py = i // ny, i % ny
    z, c = j // 2, j % 2
    other = z * 2 + (1 - c)

    row_offsets = sorted(
        [(dx, dy) for dx in range(nx) for dy in range(ny) if (dx, dy) != (0, 0)],
        key=lambda d: -(ring(d[0], nx) + ring(d[1], ny)),
    )

    def row_peer(d):
        return lax.rem(px + d[0], nx) * ny + lax.rem(py + d[1], ny)

    def row_index(d):
        return d[0] * ny + d[1]

    def col_of(dz):
        return lax.rem(z + dz, nz) * 2 + c

    load = pltpu.make_async_copy(tiles_ref.at[0, 0], a_buf, a_sem)
    load.start()

    barrier = pltpu.get_barrier_semaphore()
    for d in row_offsets:
        pl.semaphore_signal(barrier, inc=1, device_id={"row": row_peer(d)})
    for o in range(1, n_col):
        pl.semaphore_signal(barrier, inc=1, device_id={"col": lax.rem(j + o, n_col)})

    def exchange_copy(par, d):
        o = row_peer(d)
        return pltpu.make_async_remote_copy(
            src_ref=p_buf.at[par, pl.ds(o * ROW_CAP, ROW_CAP)],
            dst_ref=inc_buf[par].at[pl.ds(i * ROW_CAP, ROW_CAP)],
            send_sem=es_sem.at[par, row_index(d)],
            recv_sem=er_sem.at[par, row_index(d)],
            device_id={"row": o},
        )

    def exchange_start(par):
        for d in row_offsets:
            exchange_copy(par, d).start()
        inc_buf[par][pl.ds(i * ROW_CAP, ROW_CAP)] = p_buf[par, pl.ds(i * ROW_CAP, ROW_CAP)]

    def exchange_wait(par):
        for d in reversed(row_offsets):
            exchange_copy(par, d).wait_recv()

    def exchange_done(par):
        for d in row_offsets:
            exchange_copy(par, d).wait_send()

    def rank_copy(d):
        o = row_peer(d)
        return pltpu.make_async_remote_copy(
            src_ref=rank_v.at[o // per_half],
            dst_ref=ctab_v.at[i],
            send_sem=cs_sem.at[row_index(d)],
            recv_sem=cr_sem.at[row_index(d)],
            device_id={"row": o},
        )

    def weight_copy(d):
        return pltpu.make_async_remote_copy(
            src_ref=w_row,
            dst_ref=w_all.at[pl.ds(i * pb, pb)],
            send_sem=ws_sem.at[row_index(d)],
            recv_sem=wr_sem.at[row_index(d)],
            device_id={"row": row_peer(d)},
        )

    def u_copy(o):
        dest = lax.rem(j + o, n_col)
        return pltpu.make_async_remote_copy(
            src_ref=u_send.at[pl.ds(dest * pb, pb)],
            dst_ref=u_in.at[j],
            send_sem=us_sem.at[o],
            recv_sem=ur_sem.at[o],
            device_id={"col": dest},
        )

    def gather_copy(par, source, dest, sem):
        piece = g_buf[par].at[pl.ds(source * pb, pb)]
        return pltpu.make_async_remote_copy(
            src_ref=piece,
            dst_ref=piece,
            send_sem=gs_sem.at[par, sem],
            recv_sem=gr_sem.at[par, source],
            device_id={"col": dest},
        )

    two_phase = nz == 8
    direct = [nz - 2, 2, nz - 1, 1] if two_phase else list(range(1, nz))
    sends = 15 if two_phase else 2 * nz - 1

    def gather_start(par):
        for k, dz in enumerate(direct):
            gather_copy(par, j, col_of(dz), k).start()
        gather_copy(par, j, other, len(direct)).start()

    def arrived(par, source):
        gather_copy(par, source, other, 0).wait_recv()

    far = 2 + 4 * (1 - c)

    def gather_middle(par):
        if two_phase:
            arrived(par, col_of(6))
            gather_copy(par, col_of(6), col_of(1), 5).start()
            arrived(par, col_of(2))
            gather_copy(par, col_of(2), col_of(7), 6).start()
            gather_copy(par, col_of(8 - far), col_of(far), 7).start()
            gather_copy(par, col_of(6), other, 8).start()
            gather_copy(par, col_of(2), other, 9).start()

    def gather_wait(par):
        rest = [1, 7, 3, 5, 4] if two_phase else direct
        for k, dz in enumerate(rest):
            arrived(par, col_of(dz))
            gather_copy(par, col_of(dz), other, sends - len(rest) + k).start()
        for dz in [0, 1, nz - 1, 2, nz - 2, 3, nz - 3, 4] if two_phase else range(nz):
            arrived(par, lax.rem(z + dz, nz) * 2 + (1 - c))

    def gather_done(par):
        for sem in range(sends):
            gather_copy(par, j, other, sem).wait_send()

    def ar_row(n, d):
        return pltpu.make_async_remote_copy(
            src_ref=st_a.at[n], dst_ref=ar_a.at[n, i],
            send_sem=sa_sem.at[n, row_index(d)], recv_sem=ra_sem.at[n, row_index(d)],
            device_id={"row": row_peer(d)},
        )

    def ar_col(n, o):
        return pltpu.make_async_remote_copy(
            src_ref=st_b.at[n], dst_ref=ar_b.at[n, j],
            send_sem=sb_sem.at[n, o], recv_sem=rb_sem.at[n, o],
            device_id={"col": lax.rem(j + o, n_col)},
        )

    def tree(op, parts):
        while len(parts) > 1:
            parts = [functools.reduce(op, parts[k : k + 2]) for k in range(0, len(parts), 2)]
        return parts[0]

    def ar_start(n, value):
        st_a[n] = value
        ar_a[n, i] = value
        for d in row_offsets:
            ar_row(n, d).start()

    def ar_middle(n, op):
        for d in reversed(row_offsets):
            ar_row(n, d).wait_recv()
        value = tree(op, [ar_a[n, s] for s in range(n_row)])
        st_b[n] = value
        ar_b[n, j] = value
        for o in range(1, n_col):
            ar_col(n, o).start()

    def ar_end(n, op):
        for o in range(1, n_col):
            ar_col(n, o).wait_recv()
        value = tree(op, [ar_b[n, s] for s in range(n_col)])
        for d in row_offsets:
            ar_row(n, d).wait_send()
        for o in range(1, n_col):
            ar_col(n, o).wait_send()
        return value

    def scale_of(total):
        return nodes / jnp.broadcast_to(jnp.sum(total, axis=1, keepdims=True), (K, BLOCK))

    seed_sum = jnp.zeros((K, BLOCK), F32)
    for b in range(pb):
        seed = seeds_ref[:, b * BLOCK : (b + 1) * BLOCK].astype(F32)
        seed_sum += seed
        s_all[j * pb + b] = seed
    y_buf[tile_total] = jnp.zeros((K, BLOCK), F32)
    for par in range(2):
        inc_buf[par][slots] = jnp.zeros((K, BLOCK), F32)
    w_all[row_blocks : row_blocks + 8] = jnp.zeros((8, BLOCK), F32)

    sub = lax.broadcasted_iota(I32, (tile_total, 128), 0)
    lane = lax.broadcasted_iota(I32, (tile_total, 128), 1)
    count = counts_ref[0, 0]
    lane_row = lax.broadcasted_iota(I32, (1, 128), 1)
    key_r = jnp.where(lane_row < count, rows_ref[0], DEAD)
    key_rr = jnp.broadcast_to(key_r, (tile_total, 128))
    cols_rr = jnp.broadcast_to(cols_ref[0], (tile_total, 128))

    def lanes(value):
        return jnp.sum(value, axis=1, keepdims=True)

    def subs(value):
        return jnp.sum(value, axis=0, keepdims=True)

    def pick_if(mask, value):
        return jnp.where(mask, value, 0)

    key_c = lanes(pick_if(sub == lane, key_rr))
    cols_c = lanes(pick_if(sub == lane, cols_rr))
    key_cc = jnp.broadcast_to(key_c, (tile_total, 128))
    same = key_rr == key_cc
    before = lanes(pick_if(same & (lane < sub), 1))
    pos_c = before + lanes(pick_if(key_rr < key_cc, 1))
    last_c = lanes(pick_if(key_rr <= key_cc, 1)) - 1
    first_c = pick_if((before == 0) & (key_c < DEAD), 1)
    before_r = subs(pick_if(same & (sub < lane), 1))
    first_r = pick_if((before_r == 0) & (key_r < DEAD), 1)
    shift = pb.bit_length() - 1
    owner_c = key_c >> shift
    owner_r = key_r >> shift
    rank_c = lanes(
        pick_if((owner_r == owner_c) & (key_rr < key_cc), jnp.broadcast_to(first_r, sub.shape))
    )
    order = pos_c == lane
    slot_c = owner_c * ROW_CAP + rank_c
    chosen = slot_c == lane
    tab_v[0] = subs(pick_if(order, sub))
    tab_v[1] = subs(pick_if(order, cols_c))
    tab_v[2] = subs(pick_if(order, 1 - first_c))
    tab_v[3] = (
        subs(pick_if(chosen, first_c * last_c)) + (1 - subs(pick_if(chosen, first_c))) * tile_total
    )
    tab_v[4] = jnp.where(lane_row < count, rows_ref[0], row_blocks)
    tab_v[5] = jnp.where(
        subs(pick_if(chosen, first_c)) > 0, subs(pick_if(chosen, first_c * key_c)), row_blocks
    )
    per_half = 128 // pb
    for h in range(rank_v.shape[0]):
        found = subs(pick_if(key_c == lane + 128 * h, first_c * (rank_c + 1)))
        rank_v[h] = jnp.where(found > 0, found - 1 + i * ROW_CAP, slots)
    table = pltpu.make_async_copy(tab_v, tab_s, tab_sem)
    table.start()
    table.wait()
    load.wait()
    ctab_v[i] = rank_v[i // per_half]

    def transpose(at, carry):
        for u in range(8):
            t = at * 8 + u
            t_buf[t] = a_buf[within(tab_s[0, 0, t], tile_total - 1)].T
        return carry

    group = min(8, slots)

    def products(par, ones):
        def step(at, acc):
            for u in range(UNROLL):
                t = at * UNROLL + u
                if ones:
                    x = jnp.ones((K, BLOCK), BF16)
                else:
                    x = g_buf[par][within(tab_s[1, 0, t], col_blocks - 1)]
                y = jnp.dot(x, t_buf[t], preferred_element_type=F32)
                acc = acc * tab_s[2, 0, t].astype(F32) + y
                y_buf[t] = acc
            return acc

        lax.fori_loop(0, tile_total // UNROLL, step, jnp.zeros((K, BLOCK), F32))

        def pick(at, carry):
            for u in range(group):
                q = at * group + u
                p_buf[par, q] = y_buf[within(tab_s[3, 0, q], tile_total)]
            return carry

        lax.fori_loop(0, slots // group, pick, 0)

    def received(par, b):
        at = lax.rem(i, per_half) * pb + b
        return tree(
            jnp.add, [inc_buf[par][within(ctab_s[s, 0, at], slots)] for s in range(n_row)]
        )

    def transposed_products():
        sub8 = lax.broadcasted_iota(I32, (K, BLOCK), 0)

        def step(at, carry):
            for u in range(UNROLL):
                t = at * UNROLL + u
                w = w_all[pl.ds(within(tab_s[4, 0, t], row_blocks), 1), :]
                high, middle, low = (part.astype(F32) for part in split(w))
                rows = jnp.where(sub8 == 0, high, jnp.where(sub8 == 1, middle, low))
                rows = jnp.where(sub8 < 3, rows, 0.0).astype(BF16)
                y = jnp.dot(rows, a_buf[t], preferred_element_type=F32)
                ut_buf[pl.ds(t, 1), :] = jnp.sum(y, axis=0, keepdims=True)
            return carry

        lax.fori_loop(0, tile_total // UNROLL, step, 0)
        block_id = lax.broadcasted_iota(I32, (col_blocks, 128), 0)
        hot = jnp.where(block_id == cols_ref[0], 1.0, 0.0).astype(BF16)
        u_send[...] = sum(
            jnp.dot(hot, part, preferred_element_type=F32) for part in split(ut_buf[...])
        )

    def weighted(q0, carry):
        for u in range(group):
            q = q0 * group + u
            w = w_all[pl.ds(within(tab_s[5, 0, q], row_blocks), 1), :]
            carry += p_buf[0, q] * w
        return carry

    lax.fori_loop(0, tile_total // 8, transpose, 0)
    products(1, True)
    pl.semaphore_wait(barrier, n_row + n_col - 2)
    gather_start(2)
    ar_start(0, seed_sum)
    for d in row_offsets:
        rank_copy(d).start()
    exchange_start(1)
    gather_middle(2)
    ar_middle(0, jnp.add)
    for d in row_offsets:
        rank_copy(d).wait_recv()
    ctable = pltpu.make_async_copy(ctab_v, ctab_s, tab_sem)
    ctable.start()
    ctable.wait()
    exchange_wait(1)

    def degrees(b, carry):
        w = 1.0 / (received(1, b) + 1.0)
        w_buf[b] = w
        w_row[pl.ds(b, 1), :] = w[0:1]
        return carry

    lax.fori_loop(0, pb, degrees, 0)
    for d in row_offsets:
        weight_copy(d).start()
    w_all[pl.ds(i * pb, pb)] = w_row[...]
    gather_wait(2)
    seed_scale = scale_of(ar_end(0, jnp.add))

    def first_half(at, carry):
        for u in range(8):
            g_even[at * 8 + u] = (s_all[at * 8 + u] * seed_scale).astype(BF16)
        return carry

    lax.fori_loop(0, col_blocks // 8, first_half, 0)
    own_total = jnp.zeros((K, BLOCK), F32)
    for b in range(pb):
        v = s_all[j * pb + b] * seed_scale
        v_buf[b] = v
        own_total += v * w_buf[b]
    products(0, False)
    for d in reversed(row_offsets):
        weight_copy(d).wait_recv()
    ar_start(1, lax.fori_loop(0, slots // group, weighted, own_total))
    exchange_start(0)
    transposed_products()
    for o in range(1, n_col):
        u_copy(o).start()
    u_in[j] = u_send[pl.ds(j * pb, pb)]
    ar_middle(1, jnp.add)
    gather_done(2)
    exchange_done(1)
    for d in row_offsets:
        rank_copy(d).wait_send()
    for o in range(1, n_col):
        u_copy(o).wait_recv()
    u_buf[...] = tree(jnp.add, [u_in[s] for s in range(n_col)])

    changes = []
    for it in range(ITERS):
        par = it % 2
        if it > 0:
            gather_middle(par)
            gather_wait(par)
            ar_middle(it + 1, jnp.add)
            products(par, False)
            exchange_start(par)
            gather_done(par)
        exchange_wait(par)
        factor = scale_of(ar_end(it + 1, jnp.add))

        def advance_one(b, carry):
            change, total = carry
            old = v_buf[b]
            v = (received(par, b) + old) * w_buf[b] * factor
            change = jnp.maximum(change, jnp.abs(v - old))
            if it < ITERS - 1:
                v_buf[b] = v
                half = v.astype(BF16)
                g_buf[1 - par][j * pb + b] = half
                total += half.astype(F32) * u_buf[pl.ds(b, 1), :] + v * w_buf[b]
            else:
                raw_buf[b] = v
            return change, total

        def advance(at, carry):
            for u in range(4):
                carry = advance_one(at * 4 + u, carry)
            return carry

        blank = jnp.zeros((K, BLOCK), F32)
        change, total = lax.fori_loop(0, pb // 4, advance, (blank, blank))
        if it < ITERS - 1:
            gather_start(1 - par)
            ar_start(it + 2, total)
        exchange_done(par)
        if it == 0:
            for d in row_offsets:
                weight_copy(d).wait_send()
            for o in range(1, n_col):
                u_copy(o).wait_send()
        changes.append(jnp.max(change, axis=1, keepdims=True))

    sub8 = lax.broadcasted_iota(I32, (K, BLOCK), 0)
    lane8 = lax.broadcasted_iota(I32, (K, BLOCK), 1)
    packed = jnp.zeros((K, BLOCK), F32)
    for it in range(ITERS):
        as_row = jnp.sum(jnp.where(sub8 == lane8, changes[it], 0.0), axis=0, keepdims=True)
        packed = jnp.where(sub8 == it, as_row, packed)
    last = ITERS + 1
    ar_start(last, packed)
    for b in range(pb):
        out_ref[:, b * BLOCK : (b + 1) * BLOCK] = raw_buf[b]
    ar_middle(last, jnp.maximum)
    most = ar_end(last, jnp.maximum)
    deltas_ref[...] = most


def finish(out_in, deltas_in, out_ref, deltas_ref):
    out_ref[...] = out_in[...]
    deltas_ref[...] = deltas_in[0:ITERS, 0:K]


def solution(mesh, shape=(4, 4, 8)):
    nx, ny, nz = shape

    def on_device(tiles, block_rows, block_cols, counts, seeds):
        n_row, n_col = nx * ny, nz * 2
        tile_total = tiles.shape[2]
        piece = seeds.shape[1]
        pb = piece // BLOCK
        slots = n_row * ROW_CAP
        halves = max(1, n_row * pb // 128)
        nodes = float(piece * n_row * n_col)
        dma = pltpu.SemaphoreType.DMA
        reductions = ITERS + 2
        body = functools.partial(kernel, nx, ny, nz, pb, nodes)
        vmem = pl.BlockSpec(memory_space=pltpu.VMEM)
        out, most = pl.pallas_call(
            body,
            out_shape=(
                jax.ShapeDtypeStruct((K, piece), F32),
                jax.ShapeDtypeStruct((K, BLOCK), F32),
            ),
            in_specs=[
                pl.BlockSpec(memory_space=pl.ANY), vmem, vmem,
                pl.BlockSpec(memory_space=pltpu.SMEM), vmem,
            ],
            out_specs=(vmem, vmem),
            scratch_shapes=[
                pltpu.VMEM((tile_total, BLOCK, BLOCK), BF16),
                pltpu.VMEM((tile_total, BLOCK, BLOCK), BF16),
                pltpu.VMEM((n_col * pb, K, BLOCK), BF16),
                pltpu.VMEM((n_col * pb, K, BLOCK), BF16),
                pltpu.VMEM((n_col * pb, K, BLOCK), F32),
                pltpu.VMEM((tile_total + 1, K, BLOCK), F32),
                pltpu.VMEM((2, slots, K, BLOCK), F32),
                pltpu.VMEM((slots + 1, K, BLOCK), F32),
                pltpu.VMEM((slots + 1, K, BLOCK), F32),
                pltpu.VMEM((pb, K, BLOCK), F32),
                pltpu.VMEM((pb, K, BLOCK), F32),
                pltpu.VMEM((pb, K, BLOCK), F32),
                pltpu.VMEM((pb, BLOCK), F32),
                pltpu.VMEM((n_row * pb + 8, BLOCK), F32),
                pltpu.VMEM((tile_total, BLOCK), F32),
                pltpu.VMEM((n_col * pb, BLOCK), F32),
                pltpu.VMEM((n_col, pb, BLOCK), F32),
                pltpu.VMEM((pb, BLOCK), F32),
                pltpu.VMEM((6, 1, 128), I32),
                pltpu.SMEM((6, 1, 128), I32),
                pltpu.VMEM((halves, 1, 128), I32),
                pltpu.VMEM((n_row, 1, 128), I32),
                pltpu.SMEM((n_row, 1, 128), I32),
                pltpu.VMEM((reductions, n_row, K, BLOCK), F32),
                pltpu.VMEM((reductions, n_col, K, BLOCK), F32),
                pltpu.VMEM((reductions, K, BLOCK), F32),
                pltpu.VMEM((reductions, K, BLOCK), F32),
                dma, dma,
                dma((3, n_col)), dma((3, 2 * nz)),
                dma((2, n_row)), dma((2, n_row)),
                dma((n_row,)), dma((n_row,)),
                dma((reductions, n_row)), dma((reductions, n_row)),
                dma((reductions, n_col)), dma((reductions, n_col)),
                dma((n_row,)), dma((n_row,)),
                dma((n_col,)), dma((n_col,)),
            ],
            compiler_params=pltpu.CompilerParams(collective_id=0, has_side_effects=True),
        )(tiles, block_rows[0], block_cols[0], counts, seeds)
        return pl.pallas_call(
            finish,
            out_shape=(
                jax.ShapeDtypeStruct((K, piece), F32),
                jax.ShapeDtypeStruct((ITERS, K), F32),
            ),
            in_specs=[vmem, vmem],
            out_specs=(vmem, vmem),
        )(out, most)

    return jax.shard_map(
        on_device,
        mesh=mesh,
        in_specs=(
            P("row", "col", None, None, None),
            P("row", "col", None),
            P("row", "col", None),
            P("row", "col"),
            P(None, ("col", "row")),
        ),
        out_specs=(P(None, ("col", "row")), P()),
        check_vma=False,
    )
```

```python
import functools

import jax
import jax.numpy as jnp
from jax import lax
from jax.experimental import pallas as pl
from jax.experimental.pallas import tpu as pltpu
from jax.sharding import PartitionSpec as P

BLOCK = 128
ITERS = 4
ROW_CAP = 4
K = 8
UNROLL = 64
DEAD = 1024
F32 = jnp.float32
BF16 = jnp.bfloat16
I32 = jnp.int32


def within(index, most):
    return jnp.minimum(jnp.maximum(index, 0), most)


def ring(delta, size):
    return min(delta % size, -delta % size)


def split(value):
    high = value.astype(BF16)
    rest = value - high.astype(F32)
    middle = rest.astype(BF16)
    low = (rest - middle.astype(F32)).astype(BF16)
    return high, middle, low


def kernel(
    nx, ny, nz, pb, nodes,
    tiles_ref, rows_hbm, cols_hbm, counts_hbm, seeds_hbm,
    out_ref, deltas_ref,
    rows_ref, cols_ref, counts_ref, seeds_ref,
    a_buf, t_buf, g_even, g_odd, s_all, y_buf, p_buf, inc_even, inc_odd, v_buf, raw_buf, w_buf,
    p_deg, inc_deg, w_row, w_all, ut_buf, u_send, u_in, u_buf,
    tab_v, tab_s, rank_v, ctab_v, ctab_s, ar_a, ar_b, st_a, st_b,
    a_sem, tab_sem, gr_sem, gs_sem, er_sem, es_sem, cr_sem, cs_sem, ra_sem, sa_sem, rb_sem, sb_sem,
    wr_sem, ws_sem, ur_sem, us_sem, in_sem,
):
    n_row, n_col = nx * ny, nz * 2
    g_buf, inc_buf = (g_even, g_odd, s_all), (inc_even, inc_odd)
    tile_total = a_buf.shape[0]
    slots = n_row * ROW_CAP
    row_blocks, col_blocks = n_row * pb, n_col * pb
    i = lax.axis_index("row")
    j = lax.axis_index("col")
    px, py = i // ny, i % ny
    z, c = j // 2, j % 2
    other = z * 2 + (1 - c)

    row_offsets = sorted(
        [(dx, dy) for dx in range(nx) for dy in range(ny) if (dx, dy) != (0, 0)],
        key=lambda d: -(ring(d[0], nx) + ring(d[1], ny)),
    )

    def row_peer(d):
        return lax.rem(px + d[0], nx) * ny + lax.rem(py + d[1], ny)

    def row_index(d):
        return d[0] * ny + d[1]

    def col_of(dz):
        return lax.rem(z + dz, nz) * 2 + c

    small = [
        pltpu.make_async_copy(source, target, in_sem.at[k])
        for k, (source, target) in enumerate(
            [
                (seeds_hbm, seeds_ref),
                (rows_hbm, rows_ref),
                (cols_hbm, cols_ref),
                (counts_hbm, counts_ref),
            ]
        )
    ]
    for copy in small:
        copy.start()
    barrier = pltpu.get_barrier_semaphore()
    for d in row_offsets:
        pl.semaphore_signal(barrier, inc=1, device_id={"row": row_peer(d)})
    for o in range(1, n_col):
        pl.semaphore_signal(barrier, inc=1, device_id={"col": lax.rem(j + o, n_col)})
    load = pltpu.make_async_copy(tiles_ref.at[0, 0], a_buf, a_sem)
    load.start()

    def exchange_copy(par, d):
        o = row_peer(d)
        there, here = pl.ds(o * ROW_CAP, ROW_CAP), pl.ds(i * ROW_CAP, ROW_CAP)
        sem = 2 if par is None else par
        return pltpu.make_async_remote_copy(
            src_ref=p_deg.at[there] if par is None else p_buf.at[par, there],
            dst_ref=inc_deg.at[here] if par is None else inc_buf[par].at[here],
            send_sem=es_sem.at[sem, row_index(d)],
            recv_sem=er_sem.at[sem, row_index(d)],
            device_id={"row": o},
        )

    def exchange_start(par):
        for d in row_offsets:
            exchange_copy(par, d).start()
        here = pl.ds(i * ROW_CAP, ROW_CAP)
        if par is None:
            inc_deg[here] = p_deg[here]
        else:
            inc_buf[par][here] = p_buf[par, here]

    def exchange_wait(par):
        for d in reversed(row_offsets):
            exchange_copy(par, d).wait_recv()

    def exchange_done(par):
        for d in row_offsets:
            exchange_copy(par, d).wait_send()

    def rank_copy(d):
        o = row_peer(d)
        return pltpu.make_async_remote_copy(
            src_ref=rank_v.at[o // per_half],
            dst_ref=ctab_v.at[i],
            send_sem=cs_sem.at[row_index(d)],
            recv_sem=cr_sem.at[row_index(d)],
            device_id={"row": o},
        )

    def weight_copy(d):
        return pltpu.make_async_remote_copy(
            src_ref=w_row,
            dst_ref=w_all.at[pl.ds(i * pb, pb)],
            send_sem=ws_sem.at[row_index(d)],
            recv_sem=wr_sem.at[row_index(d)],
            device_id={"row": row_peer(d)},
        )

    def u_copy(o):
        dest = lax.rem(j + o, n_col)
        return pltpu.make_async_remote_copy(
            src_ref=u_send.at[pl.ds(dest * pb, pb)],
            dst_ref=u_in.at[j],
            send_sem=us_sem.at[o],
            recv_sem=ur_sem.at[o],
            device_id={"col": dest},
        )

    def gather_copy(par, source, dest, sem):
        piece = g_buf[par].at[pl.ds(source * pb, pb)]
        return pltpu.make_async_remote_copy(
            src_ref=piece,
            dst_ref=piece,
            send_sem=gs_sem.at[par, sem],
            recv_sem=gr_sem.at[par, source],
            device_id={"col": dest},
        )

    two_phase = nz == 8
    direct = [nz - 2, 2, nz - 1, 1] if two_phase else list(range(1, nz))
    sends = 15 if two_phase else 2 * nz - 1

    def gather_start(par):
        for k, dz in enumerate(direct):
            gather_copy(par, j, col_of(dz), k).start()
        gather_copy(par, j, other, len(direct)).start()

    def arrived(par, source):
        gather_copy(par, source, other, 0).wait_recv()

    far = 2 + 4 * (1 - c)

    def gather_middle(par):
        if two_phase:
            arrived(par, col_of(6))
            gather_copy(par, col_of(6), col_of(1), 5).start()
            arrived(par, col_of(2))
            gather_copy(par, col_of(2), col_of(7), 6).start()
            gather_copy(par, col_of(8 - far), col_of(far), 7).start()
            gather_copy(par, col_of(6), other, 8).start()
            gather_copy(par, col_of(2), other, 9).start()

    def gather_wait(par):
        rest = [1, 7, 3, 5, 4] if two_phase else direct
        for k, dz in enumerate(rest):
            arrived(par, col_of(dz))
            gather_copy(par, col_of(dz), other, sends - len(rest) + k).start()
        for dz in [0, 1, nz - 1, 2, nz - 2, 3, nz - 3, 4] if two_phase else range(nz):
            arrived(par, lax.rem(z + dz, nz) * 2 + (1 - c))

    def gather_done(par):
        for sem in range(sends):
            gather_copy(par, j, other, sem).wait_send()

    def ar_row(n, d):
        return pltpu.make_async_remote_copy(
            src_ref=st_a.at[n], dst_ref=ar_a.at[n, i],
            send_sem=sa_sem.at[n, row_index(d)], recv_sem=ra_sem.at[n, row_index(d)],
            device_id={"row": row_peer(d)},
        )

    def ar_col(n, o):
        return pltpu.make_async_remote_copy(
            src_ref=st_b.at[n], dst_ref=ar_b.at[n, j],
            send_sem=sb_sem.at[n, o], recv_sem=rb_sem.at[n, o],
            device_id={"col": lax.rem(j + o, n_col)},
        )

    def tree(op, parts):
        while len(parts) > 1:
            parts = [functools.reduce(op, parts[k : k + 2]) for k in range(0, len(parts), 2)]
        return parts[0]

    def ar_start(n, value):
        st_a[n] = value
        ar_a[n, i] = value
        for d in row_offsets:
            ar_row(n, d).start()

    def ar_middle(n, op):
        for d in reversed(row_offsets):
            ar_row(n, d).wait_recv()
        value = tree(op, [ar_a[n, s] for s in range(n_row)])
        st_b[n] = value
        ar_b[n, j] = value
        for o in range(1, n_col):
            ar_col(n, o).start()

    def ar_end(n, op):
        for o in range(1, n_col):
            ar_col(n, o).wait_recv()
        value = tree(op, [ar_b[n, s] for s in range(n_col)])
        for d in row_offsets:
            ar_row(n, d).wait_send()
        for o in range(1, n_col):
            ar_col(n, o).wait_send()
        return value

    def scale_of(total):
        return nodes / jnp.broadcast_to(jnp.sum(total, axis=1, keepdims=True), (K, BLOCK))

    y_buf[tile_total] = jnp.zeros((K, BLOCK), F32)
    for par in range(2):
        inc_buf[par][slots] = jnp.zeros((K, BLOCK), F32)
    w_all[row_blocks] = jnp.zeros((1, BLOCK), F32)
    inc_deg[slots] = jnp.zeros((1, BLOCK), F32)
    small[0].wait()
    seed_sum = jnp.zeros((K, BLOCK), F32)
    for b in range(pb):
        seed = seeds_ref[:, b * BLOCK : (b + 1) * BLOCK].astype(F32)
        seed_sum += seed
        s_all[j * pb + b] = seeds_ref[:, b * BLOCK : (b + 1) * BLOCK].astype(jnp.int16)

    pl.semaphore_wait(barrier, n_row + n_col - 2)
    gather_start(2)
    ar_start(0, seed_sum)
    for copy in small[1:]:
        copy.wait()

    sub = lax.broadcasted_iota(I32, (tile_total, 128), 0)
    lane = lax.broadcasted_iota(I32, (tile_total, 128), 1)
    count = counts_ref[...]
    lane_row = lax.broadcasted_iota(I32, (1, 128), 1)
    key_r = jnp.where(lane_row < count, rows_ref[...], DEAD)
    key_rr = jnp.broadcast_to(key_r, (tile_total, 128))
    cols_rr = jnp.broadcast_to(cols_ref[...], (tile_total, 128))

    def lanes(value):
        return jnp.sum(value, axis=1, keepdims=True)

    def subs(value):
        return jnp.sum(value, axis=0, keepdims=True)

    def pick_if(mask, value):
        return jnp.where(mask, value, 0)

    key_c = lanes(pick_if(sub == lane, key_rr))
    cols_c = lanes(pick_if(sub == lane, cols_rr))
    key_cc = jnp.broadcast_to(key_c, (tile_total, 128))
    same = key_rr == key_cc
    before = lanes(pick_if(same & (lane < sub), 1))
    pos_c = before + lanes(pick_if(key_rr < key_cc, 1))
    last_c = lanes(pick_if(key_rr <= key_cc, 1)) - 1
    first_c = pick_if((before == 0) & (key_c < DEAD), 1)
    before_r = subs(pick_if(same & (sub < lane), 1))
    first_r = pick_if((before_r == 0) & (key_r < DEAD), 1)
    shift = pb.bit_length() - 1
    owner_c = key_c >> shift
    owner_r = key_r >> shift
    rank_c = lanes(
        pick_if((owner_r == owner_c) & (key_rr < key_cc), jnp.broadcast_to(first_r, sub.shape))
    )
    order = pos_c == lane
    slot_c = owner_c * ROW_CAP + rank_c
    chosen = slot_c == lane
    tab_v[0] = subs(pick_if(order, sub))
    tab_v[1] = subs(pick_if(order, cols_c))
    tab_v[2] = subs(pick_if(order, 1 - first_c))
    tab_v[3] = (
        subs(pick_if(chosen, first_c * last_c)) + (1 - subs(pick_if(chosen, first_c))) * tile_total
    )
    tab_v[4] = jnp.where(lane_row < count, rows_ref[...], row_blocks)
    tab_v[5] = jnp.where(
        subs(pick_if(chosen, first_c)) > 0, subs(pick_if(chosen, first_c * key_c)), row_blocks
    )
    per_half = 128 // pb
    for h in range(rank_v.shape[0]):
        found = subs(pick_if(key_c == lane + 128 * h, first_c * (rank_c + 1)))
        rank_v[h] = jnp.where(found > 0, found - 1 + i * ROW_CAP, slots)
    table = pltpu.make_async_copy(tab_v, tab_s, tab_sem)
    table.start()
    table.wait()
    load.wait()
    ctab_v[i] = rank_v[i // per_half]

    group = min(8, slots)

    def products(par, ones):
        def step(at, acc):
            for u in range(UNROLL):
                t = at * UNROLL + u
                if ones:
                    x = jnp.ones((K, BLOCK), BF16)
                    tile = a_buf[within(tab_s[0, 0, t], tile_total - 1)].T
                    t_buf[t] = tile
                else:
                    x = g_buf[par][within(tab_s[1, 0, t], col_blocks - 1)]
                    tile = t_buf[t]
                y = jnp.dot(x, tile, preferred_element_type=F32)
                acc = acc * tab_s[2, 0, t].astype(F32) + y
                y_buf[t] = acc
            return acc

        lax.fori_loop(0, tile_total // UNROLL, step, jnp.zeros((K, BLOCK), F32))

        def pick(at, carry):
            for u in range(group):
                q = at * group + u
                value = y_buf[within(tab_s[3, 0, q], tile_total)]
                if ones:
                    p_deg[q] = value[0:1]
                else:
                    p_buf[par, q] = value
            return carry

        lax.fori_loop(0, slots // group, pick, 0)

    def received(par, b):
        at = lax.rem(i, per_half) * pb + b
        source = inc_deg if par is None else inc_buf[par]
        return tree(
            jnp.add, [source[within(ctab_s[s, 0, at], slots)] for s in range(n_row)]
        )

    def transposed_products():
        sub8 = lax.broadcasted_iota(I32, (K, BLOCK), 0)

        def step(at, carry):
            for u in range(UNROLL):
                t = at * UNROLL + u
                w = w_all[within(tab_s[4, 0, t], row_blocks)]
                high, middle, low = (part.astype(F32) for part in split(w))
                rows = jnp.where(sub8 == 0, high, jnp.where(sub8 == 1, middle, low))
                rows = jnp.where(sub8 < 3, rows, 0.0).astype(BF16)
                y = jnp.dot(rows, a_buf[t], preferred_element_type=F32)
                ut_buf[pl.ds(t, 1), :] = jnp.sum(y, axis=0, keepdims=True)
            return carry

        lax.fori_loop(0, tile_total // UNROLL, step, 0)
        block_id = lax.broadcasted_iota(I32, (col_blocks, 128), 0)
        hot = jnp.where(block_id == cols_ref[...], 1.0, 0.0).astype(BF16)
        u_send[...] = sum(
            jnp.dot(hot, part, preferred_element_type=F32) for part in split(ut_buf[...])
        )

    def weighted(q0, carry):
        for u in range(group):
            q = q0 * group + u
            w = w_all[within(tab_s[5, 0, q], row_blocks)]
            carry += p_buf[0, q] * w
        return carry

    products(None, True)
    for d in row_offsets:
        rank_copy(d).start()
    exchange_start(None)
    gather_middle(2)
    ar_middle(0, jnp.add)
    for d in row_offsets:
        rank_copy(d).wait_recv()
    ctable = pltpu.make_async_copy(ctab_v, ctab_s, tab_sem)
    ctable.start()
    ctable.wait()
    exchange_wait(None)

    def degrees(at, carry):
        for u in range(4):
            b = at * 4 + u
            w = 1.0 / (received(None, b) + 1.0)
            w_buf[b] = jnp.broadcast_to(w, (K, BLOCK))
            w_row[b] = w
        return carry

    lax.fori_loop(0, pb // 4, degrees, 0)
    for d in row_offsets:
        weight_copy(d).start()
    w_all[pl.ds(i * pb, pb)] = w_row[...]
    gather_wait(2)
    seed_scale = scale_of(ar_end(0, jnp.add))

    def first_half(at, carry):
        for u in range(8):
            g_even[at * 8 + u] = (s_all[at * 8 + u].astype(I32).astype(F32) * seed_scale).astype(BF16)
        return carry

    lax.fori_loop(0, col_blocks // 8, first_half, 0)
    own_total = jnp.zeros((K, BLOCK), F32)
    for b in range(pb):
        v = seeds_ref[:, b * BLOCK : (b + 1) * BLOCK].astype(F32) * seed_scale
        v_buf[b] = v
        own_total += v * w_buf[b]
    products(0, False)
    for d in reversed(row_offsets):
        weight_copy(d).wait_recv()
    ar_start(1, lax.fori_loop(0, slots // group, weighted, own_total))
    exchange_start(0)
    transposed_products()
    for o in range(1, n_col):
        u_copy(o).start()
    u_in[j] = u_send[pl.ds(j * pb, pb)]
    ar_middle(1, jnp.add)
    gather_done(2)
    exchange_done(None)
    for d in row_offsets:
        rank_copy(d).wait_send()
    for o in range(1, n_col):
        u_copy(o).wait_recv()
    u_sum = tree(jnp.add, [u_in[s] for s in range(n_col)])
    for b in range(pb):
        u_buf[b] = u_sum[b : b + 1]

    changes = []
    for it in range(ITERS):
        par = it % 2
        if it > 0:
            gather_middle(par)
            gather_wait(par)
            ar_middle(it + 1, jnp.add)
            products(par, False)
            exchange_start(par)
            gather_done(par)
        exchange_wait(par)
        factor = scale_of(ar_end(it + 1, jnp.add))

        def advance_one(b, carry):
            change, total = carry
            old = v_buf[b]
            v = (received(par, b) + old) * w_buf[b] * factor
            change = jnp.maximum(change, jnp.abs(v - old))
            if it < ITERS - 1:
                v_buf[b] = v
                half = v.astype(BF16)
                g_buf[1 - par][j * pb + b] = half
                total += half.astype(F32) * u_buf[b] + v * w_buf[b]
            else:
                raw_buf[b] = v
            return change, total

        def advance(at, carry):
            for u in range(4):
                carry = advance_one(at * 4 + u, carry)
            return carry

        blank = jnp.zeros((K, BLOCK), F32)
        change, total = lax.fori_loop(0, pb // 4, advance, (blank, blank))
        if it < ITERS - 1:
            gather_start(1 - par)
            ar_start(it + 2, total)
        exchange_done(par)
        if it == 0:
            for d in row_offsets:
                weight_copy(d).wait_send()
            for o in range(1, n_col):
                u_copy(o).wait_send()
        changes.append(jnp.max(change, axis=1, keepdims=True))

    sub8 = lax.broadcasted_iota(I32, (K, BLOCK), 0)
    lane8 = lax.broadcasted_iota(I32, (K, BLOCK), 1)
    packed = jnp.zeros((K, BLOCK), F32)
    for it in range(ITERS):
        as_row = jnp.sum(jnp.where(sub8 == lane8, changes[it], 0.0), axis=0, keepdims=True)
        packed = jnp.where(sub8 == it, as_row, packed)
    last = ITERS + 1
    ar_start(last, packed)
    for b in range(pb):
        out_ref[:, b * BLOCK : (b + 1) * BLOCK] = raw_buf[b]
    ar_middle(last, jnp.maximum)
    most = ar_end(last, jnp.maximum)
    deltas_ref[...] = most


def finish(out_in, deltas_in, out_ref, deltas_ref):
    out_ref[...] = out_in[...]
    deltas_ref[...] = deltas_in[0:ITERS, 0:K]


def solution(mesh, shape=(4, 4, 8)):
    nx, ny, nz = shape

    def on_device(tiles, block_rows, block_cols, counts, seeds):
        n_row, n_col = nx * ny, nz * 2
        tile_total = tiles.shape[2]
        piece = seeds.shape[1]
        pb = piece // BLOCK
        slots = n_row * ROW_CAP
        halves = max(1, n_row * pb // 128)
        nodes = float(piece * n_row * n_col)
        dma = pltpu.SemaphoreType.DMA
        reductions = ITERS + 2
        body = functools.partial(kernel, nx, ny, nz, pb, nodes)
        vmem = pl.BlockSpec(memory_space=pltpu.VMEM)
        out, most = pl.pallas_call(
            body,
            out_shape=(
                jax.ShapeDtypeStruct((K, piece), F32),
                jax.ShapeDtypeStruct((K, BLOCK), F32),
            ),
            in_specs=[
                pl.BlockSpec(memory_space=pltpu.HBM) for _ in range(5)
            ],
            out_specs=(vmem, vmem),
            scratch_shapes=[
                pltpu.VMEM((1, tile_total), I32),
                pltpu.VMEM((1, tile_total), I32),
                pltpu.VMEM((1, 1), I32),
                pltpu.VMEM((K, piece), I32),
                pltpu.VMEM((tile_total, BLOCK, BLOCK), BF16),
                pltpu.VMEM((tile_total, BLOCK, BLOCK), BF16),
                pltpu.VMEM((n_col * pb, K, BLOCK), BF16),
                pltpu.VMEM((n_col * pb, K, BLOCK), BF16),
                pltpu.VMEM((n_col * pb, K, BLOCK), jnp.int16),
                pltpu.VMEM((tile_total + 1, K, BLOCK), F32),
                pltpu.VMEM((2, slots, K, BLOCK), F32),
                pltpu.VMEM((slots + 1, K, BLOCK), F32),
                pltpu.VMEM((slots + 1, K, BLOCK), F32),
                pltpu.VMEM((pb, K, BLOCK), F32),
                pltpu.VMEM((pb, K, BLOCK), F32),
                pltpu.VMEM((pb, K, BLOCK), F32),
                pltpu.VMEM((slots, 1, BLOCK), F32),
                pltpu.VMEM((slots + 1, 1, BLOCK), F32),
                pltpu.VMEM((pb, 1, BLOCK), F32),
                pltpu.VMEM((n_row * pb + 1, 1, BLOCK), F32),
                pltpu.VMEM((tile_total, BLOCK), F32),
                pltpu.VMEM((n_col * pb, BLOCK), F32),
                pltpu.VMEM((n_col, pb, BLOCK), F32),
                pltpu.VMEM((pb, 1, BLOCK), F32),
                pltpu.VMEM((6, 1, 128), I32),
                pltpu.SMEM((6, 1, 128), I32),
                pltpu.VMEM((halves, 1, 128), I32),
                pltpu.VMEM((n_row, 1, 128), I32),
                pltpu.SMEM((n_row, 1, 128), I32),
                pltpu.VMEM((reductions, n_row, K, BLOCK), F32),
                pltpu.VMEM((reductions, n_col, K, BLOCK), F32),
                pltpu.VMEM((reductions, K, BLOCK), F32),
                pltpu.VMEM((reductions, K, BLOCK), F32),
                dma, dma,
                dma((3, n_col)), dma((3, 2 * nz)),
                dma((3, n_row)), dma((3, n_row)),
                dma((n_row,)), dma((n_row,)),
                dma((reductions, n_row)), dma((reductions, n_row)),
                dma((reductions, n_col)), dma((reductions, n_col)),
                dma((n_row,)), dma((n_row,)),
                dma((n_col,)), dma((n_col,)), dma((4,)),
            ],
            compiler_params=pltpu.CompilerParams(collective_id=0, has_side_effects=True),
        )(tiles, block_rows[0], block_cols[0], counts, seeds)
        return pl.pallas_call(
            finish,
            out_shape=(
                jax.ShapeDtypeStruct((K, piece), F32),
                jax.ShapeDtypeStruct((ITERS, K), F32),
            ),
            in_specs=[vmem, vmem],
            out_specs=(vmem, vmem),
        )(out, most)

    return jax.shard_map(
        on_device,
        mesh=mesh,
        in_specs=(
            P("row", "col", None, None, None),
            P("row", "col", None),
            P("row", "col", None),
            P("row", "col"),
            P(None, ("col", "row")),
        ),
        out_specs=(P(None, ("col", "row")), P()),
        check_vma=False,
    )
```

```python
import functools

import jax
import jax.numpy as jnp
from jax import lax
from jax.experimental import pallas as pl
from jax.experimental.pallas import tpu as pltpu
from jax.sharding import PartitionSpec as P

BLOCK = 128
ITERS = 4
ROW_CAP = 4
K = 8
UNROLL = 128
DEAD = 1024
F32 = jnp.float32
BF16 = jnp.bfloat16
I32 = jnp.int32


def within(index, most):
    return jnp.minimum(jnp.maximum(index, 0), most)


def ring(delta, size):
    return min(delta % size, -delta % size)


def split(value):
    high = value.astype(BF16)
    rest = value - high.astype(F32)
    middle = rest.astype(BF16)
    low = (rest - middle.astype(F32)).astype(BF16)
    return high, middle, low


def kernel(
    nx, ny, nz, pb, nodes,
    tiles_ref, rows_hbm, cols_hbm, counts_hbm, seeds_hbm,
    out_ref, deltas_ref,
    rows_ref, cols_ref, counts_ref, seeds_ref,
    a_buf, t_buf, g_even, g_odd, s_all, y_buf, p_buf, inc_even, inc_odd, v_buf, raw_buf, w_buf,
    p_deg, inc_deg, w_row, w_all, ut_buf, u_send, u_in, u_buf,
    tab_v, tab_s, rank_v, ctab_v, ctab_s, ar_a, ar_b, st_a, st_b,
    a_sem, tab_sem, gr_sem, gs_sem, er_sem, es_sem, cr_sem, cs_sem, ra_sem, sa_sem, rb_sem, sb_sem,
    wr_sem, ws_sem, ur_sem, us_sem, in_sem,
):
    n_row, n_col = nx * ny, nz * 2
    g_buf, inc_buf = (g_even, g_odd, s_all), (inc_even, inc_odd)
    tile_total = a_buf.shape[0]
    slots = n_row * ROW_CAP
    row_blocks, col_blocks = n_row * pb, n_col * pb
    i = lax.axis_index("row")
    j = lax.axis_index("col")
    px, py = i // ny, i % ny
    z, c = j // 2, j % 2
    other = z * 2 + (1 - c)

    row_offsets = sorted(
        [(dx, dy) for dx in range(nx) for dy in range(ny) if (dx, dy) != (0, 0)],
        key=lambda d: -(ring(d[0], nx) + ring(d[1], ny)),
    )

    def row_peer(d):
        return lax.rem(px + d[0], nx) * ny + lax.rem(py + d[1], ny)

    def row_index(d):
        return d[0] * ny + d[1]

    def col_of(dz):
        return lax.rem(z + dz, nz) * 2 + c

    small = [
        pltpu.make_async_copy(source, target, in_sem.at[k])
        for k, (source, target) in enumerate(
            [
                (seeds_hbm, seeds_ref),
                (rows_hbm, rows_ref),
                (cols_hbm, cols_ref),
                (counts_hbm, counts_ref),
            ]
        )
    ]
    for copy in small:
        copy.start()
    barrier = pltpu.get_barrier_semaphore()
    for d in row_offsets:
        pl.semaphore_signal(barrier, inc=1, device_id={"row": row_peer(d)})
    for o in range(1, n_col):
        pl.semaphore_signal(barrier, inc=1, device_id={"col": lax.rem(j + o, n_col)})
    load = pltpu.make_async_copy(tiles_ref.at[0, 0], a_buf, a_sem)
    load.start()

    def exchange_copy(par, d):
        o = row_peer(d)
        there, here = pl.ds(o * ROW_CAP, ROW_CAP), pl.ds(i * ROW_CAP, ROW_CAP)
        sem = 2 if par is None else par
        return pltpu.make_async_remote_copy(
            src_ref=p_deg.at[there] if par is None else p_buf.at[par, there],
            dst_ref=inc_deg.at[here] if par is None else inc_buf[par].at[here],
            send_sem=es_sem.at[sem, row_index(d)],
            recv_sem=er_sem.at[sem, row_index(d)],
            device_id={"row": o},
        )

    def exchange_start(par):
        for d in row_offsets:
            exchange_copy(par, d).start()
        here = pl.ds(i * ROW_CAP, ROW_CAP)
        if par is None:
            inc_deg[here] = p_deg[here]
        else:
            inc_buf[par][here] = p_buf[par, here]

    def exchange_wait(par):
        for d in reversed(row_offsets):
            exchange_copy(par, d).wait_recv()

    def exchange_done(par):
        for d in row_offsets:
            exchange_copy(par, d).wait_send()

    def rank_copy(d):
        o = row_peer(d)
        return pltpu.make_async_remote_copy(
            src_ref=rank_v.at[o // per_half],
            dst_ref=ctab_v.at[i],
            send_sem=cs_sem.at[row_index(d)],
            recv_sem=cr_sem.at[row_index(d)],
            device_id={"row": o},
        )

    def weight_copy(d):
        return pltpu.make_async_remote_copy(
            src_ref=w_row,
            dst_ref=w_all.at[pl.ds(i * pb, pb)],
            send_sem=ws_sem.at[row_index(d)],
            recv_sem=wr_sem.at[row_index(d)],
            device_id={"row": row_peer(d)},
        )

    def u_copy(o):
        dest = lax.rem(j + o, n_col)
        return pltpu.make_async_remote_copy(
            src_ref=u_send.at[pl.ds(dest * pb, pb)],
            dst_ref=u_in.at[j],
            send_sem=us_sem.at[o],
            recv_sem=ur_sem.at[o],
            device_id={"col": dest},
        )

    def gather_copy(par, source, dest, sem):
        piece = g_buf[par].at[pl.ds(source * pb, pb)]
        return pltpu.make_async_remote_copy(
            src_ref=piece,
            dst_ref=piece,
            send_sem=gs_sem.at[par, sem],
            recv_sem=gr_sem.at[par, source],
            device_id={"col": dest},
        )

    two_phase = nz == 8
    direct = [nz - 2, 2, nz - 1, 1] if two_phase else list(range(1, nz))
    sends = 15 if two_phase else 2 * nz - 1

    def gather_start(par):
        for k, dz in enumerate(direct):
            gather_copy(par, j, col_of(dz), k).start()
        gather_copy(par, j, other, len(direct)).start()

    def arrived(par, source):
        gather_copy(par, source, other, 0).wait_recv()

    far = 2 + 4 * (1 - c)

    def gather_middle(par):
        if two_phase:
            arrived(par, col_of(6))
            gather_copy(par, col_of(6), col_of(1), 5).start()
            arrived(par, col_of(2))
            gather_copy(par, col_of(2), col_of(7), 6).start()
            gather_copy(par, col_of(8 - far), col_of(far), 7).start()
            gather_copy(par, col_of(6), other, 8).start()
            gather_copy(par, col_of(2), other, 9).start()

    def gather_wait(par):
        rest = [1, 7, 3, 5, 4] if two_phase else direct
        for k, dz in enumerate(rest):
            arrived(par, col_of(dz))
            gather_copy(par, col_of(dz), other, sends - len(rest) + k).start()
        for dz in [0, 1, nz - 1, 2, nz - 2, 3, nz - 3, 4] if two_phase else range(nz):
            arrived(par, lax.rem(z + dz, nz) * 2 + (1 - c))

    def gather_done(par):
        for sem in range(sends):
            gather_copy(par, j, other, sem).wait_send()

    def ar_row(n, d):
        return pltpu.make_async_remote_copy(
            src_ref=st_a.at[n], dst_ref=ar_a.at[n, i],
            send_sem=sa_sem.at[n, row_index(d)], recv_sem=ra_sem.at[n, row_index(d)],
            device_id={"row": row_peer(d)},
        )

    def ar_col(n, o):
        return pltpu.make_async_remote_copy(
            src_ref=st_b.at[n], dst_ref=ar_b.at[n, j],
            send_sem=sb_sem.at[n, o], recv_sem=rb_sem.at[n, o],
            device_id={"col": lax.rem(j + o, n_col)},
        )

    def tree(op, parts):
        while len(parts) > 1:
            parts = [functools.reduce(op, parts[k : k + 2]) for k in range(0, len(parts), 2)]
        return parts[0]

    def ar_start(n, value):
        st_a[n] = value
        ar_a[n, i] = value
        for d in row_offsets:
            ar_row(n, d).start()

    def ar_middle(n, op):
        for d in reversed(row_offsets):
            ar_row(n, d).wait_recv()
        value = tree(op, [ar_a[n, s] for s in range(n_row)])
        st_b[n] = value
        ar_b[n, j] = value
        for o in range(1, n_col):
            ar_col(n, o).start()

    def ar_end(n, op):
        for o in range(1, n_col):
            ar_col(n, o).wait_recv()
        value = tree(op, [ar_b[n, s] for s in range(n_col)])
        for d in row_offsets:
            ar_row(n, d).wait_send()
        for o in range(1, n_col):
            ar_col(n, o).wait_send()
        return value

    def scale_of(total):
        return nodes / jnp.broadcast_to(jnp.sum(total, axis=1, keepdims=True), (K, BLOCK))

    y_buf[tile_total] = jnp.zeros((K, BLOCK), F32)
    for par in range(2):
        inc_buf[par][slots] = jnp.zeros((K, BLOCK), F32)
    w_all[row_blocks] = jnp.zeros((1, BLOCK), F32)
    inc_deg[slots] = jnp.zeros((1, BLOCK), F32)
    small[0].wait()
    seed_sum = jnp.zeros((K, BLOCK), F32)
    for b in range(pb):
        seed = seeds_ref[:, b * BLOCK : (b + 1) * BLOCK].astype(F32)
        seed_sum += seed
        s_all[j * pb + b] = seeds_ref[:, b * BLOCK : (b + 1) * BLOCK].astype(jnp.int16)

    pl.semaphore_wait(barrier, n_row + n_col - 2)
    gather_start(2)
    ar_start(0, seed_sum)
    for copy in small[1:]:
        copy.wait()

    sub = lax.broadcasted_iota(I32, (tile_total, 128), 0)
    lane = lax.broadcasted_iota(I32, (tile_total, 128), 1)
    count = counts_ref[...]
    lane_row = lax.broadcasted_iota(I32, (1, 128), 1)
    key_r = jnp.where(lane_row < count, rows_ref[...], DEAD)
    key_rr = jnp.broadcast_to(key_r, (tile_total, 128))
    cols_rr = jnp.broadcast_to(cols_ref[...], (tile_total, 128))

    def lanes(value):
        return jnp.sum(value, axis=1, keepdims=True)

    def subs(value):
        return jnp.sum(value, axis=0, keepdims=True)

    def pick_if(mask, value):
        return jnp.where(mask, value, 0)

    key_c = lanes(pick_if(sub == lane, key_rr))
    cols_c = lanes(pick_if(sub == lane, cols_rr))
    key_cc = jnp.broadcast_to(key_c, (tile_total, 128))
    same = key_rr == key_cc
    before = lanes(pick_if(same & (lane < sub), 1))
    pos_c = before + lanes(pick_if(key_rr < key_cc, 1))
    last_c = lanes(pick_if(key_rr <= key_cc, 1)) - 1
    first_c = pick_if((before == 0) & (key_c < DEAD), 1)
    before_r = subs(pick_if(same & (sub < lane), 1))
    first_r = pick_if((before_r == 0) & (key_r < DEAD), 1)
    shift = pb.bit_length() - 1
    owner_c = key_c >> shift
    owner_r = key_r >> shift
    rank_c = lanes(
        pick_if((owner_r == owner_c) & (key_rr < key_cc), jnp.broadcast_to(first_r, sub.shape))
    )
    order = pos_c == lane
    slot_c = owner_c * ROW_CAP + rank_c
    chosen = slot_c == lane
    tab_v[0] = subs(pick_if(order, sub))
    tab_v[1] = subs(pick_if(order, cols_c))
    tab_v[2] = subs(pick_if(order, 1 - first_c))
    tab_v[3] = (
        subs(pick_if(chosen, first_c * last_c)) + (1 - subs(pick_if(chosen, first_c))) * tile_total
    )
    tab_v[4] = jnp.where(lane_row < count, rows_ref[...], row_blocks)
    tab_v[5] = jnp.where(
        subs(pick_if(chosen, first_c)) > 0, subs(pick_if(chosen, first_c * key_c)), row_blocks
    )
    per_half = 128 // pb
    for h in range(rank_v.shape[0]):
        found = subs(pick_if(key_c == lane + 128 * h, first_c * (rank_c + 1)))
        rank_v[h] = jnp.where(found > 0, found - 1 + i * ROW_CAP, slots)
    table = pltpu.make_async_copy(tab_v, tab_s, tab_sem)
    table.start()
    for d in row_offsets:
        rank_copy(d).start()
    table.wait()
    load.wait()
    ctab_v[i] = rank_v[i // per_half]

    def products(par, ones):
        def step(at, acc):
            for u in range(UNROLL):
                t = at * UNROLL + u
                if ones:
                    x = jnp.ones((K, BLOCK), BF16)
                    tile = a_buf[within(tab_s[0, 0, t], tile_total - 1)].T
                    t_buf[t] = tile
                else:
                    x = g_buf[par][within(tab_s[1, 0, t], col_blocks - 1)]
                    tile = t_buf[t]
                y = jnp.dot(x, tile, preferred_element_type=F32)
                acc = acc * tab_s[2, 0, t].astype(F32) + y
                y_buf[t] = acc
            return acc

        lax.fori_loop(0, tile_total // UNROLL, step, jnp.zeros((K, BLOCK), F32))

        for q in range(slots):
            value = y_buf[within(tab_s[3, 0, q], tile_total)]
            if ones:
                p_deg[q] = value[0:1]
            else:
                p_buf[par, q] = value

    def received(par, b):
        at = lax.rem(i, per_half) * pb + b
        source = inc_deg if par is None else inc_buf[par]
        return tree(
            jnp.add, [source[within(ctab_s[s, 0, at], slots)] for s in range(n_row)]
        )

    def transposed_products():
        sub8 = lax.broadcasted_iota(I32, (K, BLOCK), 0)

        def step(at, carry):
            for u in range(UNROLL):
                t = at * UNROLL + u
                w = w_all[within(tab_s[4, 0, t], row_blocks)]
                high, middle, low = (part.astype(F32) for part in split(w))
                rows = jnp.where(sub8 == 0, high, jnp.where(sub8 == 1, middle, low))
                rows = jnp.where(sub8 < 3, rows, 0.0).astype(BF16)
                y = jnp.dot(rows, a_buf[t], preferred_element_type=F32)
                ut_buf[pl.ds(t, 1), :] = jnp.sum(y, axis=0, keepdims=True)
            return carry

        lax.fori_loop(0, tile_total // UNROLL, step, 0)
        block_id = lax.broadcasted_iota(I32, (col_blocks, 128), 0)
        hot = jnp.where(block_id == cols_ref[...], 1.0, 0.0).astype(BF16)
        u_send[...] = sum(
            jnp.dot(hot, part, preferred_element_type=F32) for part in split(ut_buf[...])
        )

    def weighted(base):
        sums = [base] + [jnp.zeros((K, BLOCK), F32) for _ in range(3)]
        for q in range(slots):
            w = w_all[within(tab_s[5, 0, q], row_blocks)]
            sums[q % 4] += p_buf[0, q] * w
        return tree(jnp.add, sums)

    products(None, True)
    exchange_start(None)
    gather_middle(2)
    ar_middle(0, jnp.add)
    for d in row_offsets:
        rank_copy(d).wait_recv()
    ctable = pltpu.make_async_copy(ctab_v, ctab_s, tab_sem)
    ctable.start()
    exchange_wait(None)
    ctable.wait()

    for b in range(pb):
        w = 1.0 / (received(None, b) + 1.0)
        w_buf[b] = jnp.broadcast_to(w, (K, BLOCK))
        w_row[b] = w
    for d in row_offsets:
        weight_copy(d).start()
    w_all[pl.ds(i * pb, pb)] = w_row[...]
    gather_wait(2)
    seed_scale = scale_of(ar_end(0, jnp.add))

    def first_half(at, carry):
        for u in range(8):
            g_even[at * 8 + u] = (s_all[at * 8 + u].astype(I32).astype(F32) * seed_scale).astype(BF16)
        return carry

    lax.fori_loop(0, col_blocks // 8, first_half, 0)
    own_total = jnp.zeros((K, BLOCK), F32)
    for b in range(pb):
        v = seeds_ref[:, b * BLOCK : (b + 1) * BLOCK].astype(F32) * seed_scale
        v_buf[b] = v
        own_total += v * w_buf[b]
    products(0, False)
    for d in reversed(row_offsets):
        weight_copy(d).wait_recv()
    ar_start(1, weighted(own_total))
    exchange_start(0)
    transposed_products()
    for o in range(1, n_col):
        u_copy(o).start()
    u_in[j] = u_send[pl.ds(j * pb, pb)]
    ar_middle(1, jnp.add)
    gather_done(2)
    exchange_done(None)
    for d in row_offsets:
        rank_copy(d).wait_send()
    for o in range(1, n_col):
        u_copy(o).wait_recv()
    u_sum = tree(jnp.add, [u_in[s] for s in range(n_col)])
    for b in range(pb):
        u_buf[b] = u_sum[b : b + 1]

    changes = []
    for it in range(ITERS):
        par = it % 2
        if it > 0:
            gather_middle(par)
            gather_wait(par)
            ar_middle(it + 1, jnp.add)
            products(par, False)
            exchange_start(par)
            gather_done(par)
        exchange_wait(par)
        factor = scale_of(ar_end(it + 1, jnp.add))

        def advance_one(b, carry):
            change, total = carry
            old = v_buf[b]
            v = (received(par, b) + old) * w_buf[b] * factor
            change = jnp.maximum(change, jnp.abs(v - old))
            if it < ITERS - 1:
                v_buf[b] = v
                half = v.astype(BF16)
                g_buf[1 - par][j * pb + b] = half
                total += half.astype(F32) * u_buf[b] + v * w_buf[b]
            else:
                raw_buf[b] = v
            return change, total

        blank = jnp.zeros((K, BLOCK), F32)
        change, total = blank, blank
        for b in range(pb):
            change, total = advance_one(b, (change, total))
        if it < ITERS - 1:
            gather_start(1 - par)
            ar_start(it + 2, total)
        exchange_done(par)
        if it == 0:
            for d in row_offsets:
                weight_copy(d).wait_send()
            for o in range(1, n_col):
                u_copy(o).wait_send()
        changes.append(jnp.max(change, axis=1, keepdims=True))

    sub8 = lax.broadcasted_iota(I32, (K, BLOCK), 0)
    lane8 = lax.broadcasted_iota(I32, (K, BLOCK), 1)
    packed = jnp.zeros((K, BLOCK), F32)
    for it in range(ITERS):
        as_row = jnp.sum(jnp.where(sub8 == lane8, changes[it], 0.0), axis=0, keepdims=True)
        packed = jnp.where(sub8 == it, as_row, packed)
    last = ITERS + 1
    ar_start(last, packed)
    for b in range(pb):
        out_ref[:, b * BLOCK : (b + 1) * BLOCK] = raw_buf[b]
    ar_middle(last, jnp.maximum)
    most = ar_end(last, jnp.maximum)
    deltas_ref[...] = most[0:ITERS, 0:K]


def solution(mesh, shape=(4, 4, 8)):
    nx, ny, nz = shape

    def on_device(tiles, block_rows, block_cols, counts, seeds):
        n_row, n_col = nx * ny, nz * 2
        tile_total = tiles.shape[2]
        piece = seeds.shape[1]
        pb = piece // BLOCK
        slots = n_row * ROW_CAP
        halves = max(1, n_row * pb // 128)
        nodes = float(piece * n_row * n_col)
        dma = pltpu.SemaphoreType.DMA
        reductions = ITERS + 2
        body = functools.partial(kernel, nx, ny, nz, pb, nodes)
        vmem = pl.BlockSpec(memory_space=pltpu.VMEM)
        return pl.pallas_call(
            body,
            out_shape=(
                pltpu.VMEM((K, piece), F32),
                pltpu.VMEM((ITERS, K), F32),
            ),
            in_specs=[
                pl.BlockSpec(memory_space=pltpu.HBM) for _ in range(5)
            ],
            out_specs=(vmem, vmem),
            scratch_shapes=[
                pltpu.VMEM((1, tile_total), I32),
                pltpu.VMEM((1, tile_total), I32),
                pltpu.VMEM((1, 1), I32),
                pltpu.VMEM((K, piece), I32),
                pltpu.VMEM((tile_total, BLOCK, BLOCK), BF16),
                pltpu.VMEM((tile_total, BLOCK, BLOCK), BF16),
                pltpu.VMEM((n_col * pb, K, BLOCK), BF16),
                pltpu.VMEM((n_col * pb, K, BLOCK), BF16),
                pltpu.VMEM((n_col * pb, K, BLOCK), jnp.int16),
                pltpu.VMEM((tile_total + 1, K, BLOCK), F32),
                pltpu.VMEM((2, slots, K, BLOCK), F32),
                pltpu.VMEM((slots + 1, K, BLOCK), F32),
                pltpu.VMEM((slots + 1, K, BLOCK), F32),
                pltpu.VMEM((pb, K, BLOCK), F32),
                pltpu.VMEM((pb, K, BLOCK), F32),
                pltpu.VMEM((pb, K, BLOCK), F32),
                pltpu.VMEM((slots, 1, BLOCK), F32),
                pltpu.VMEM((slots + 1, 1, BLOCK), F32),
                pltpu.VMEM((pb, 1, BLOCK), F32),
                pltpu.VMEM((n_row * pb + 1, 1, BLOCK), F32),
                pltpu.VMEM((tile_total, BLOCK), F32),
                pltpu.VMEM((n_col * pb, BLOCK), F32),
                pltpu.VMEM((n_col, pb, BLOCK), F32),
                pltpu.VMEM((pb, 1, BLOCK), F32),
                pltpu.VMEM((6, 1, 128), I32),
                pltpu.SMEM((6, 1, 128), I32),
                pltpu.VMEM((halves, 1, 128), I32),
                pltpu.VMEM((n_row, 1, 128), I32),
                pltpu.SMEM((n_row, 1, 128), I32),
                pltpu.VMEM((reductions, n_row, K, BLOCK), F32),
                pltpu.VMEM((reductions, n_col, K, BLOCK), F32),
                pltpu.VMEM((reductions, K, BLOCK), F32),
                pltpu.VMEM((reductions, K, BLOCK), F32),
                dma, dma,
                dma((3, n_col)), dma((3, 2 * nz)),
                dma((3, n_row)), dma((3, n_row)),
                dma((n_row,)), dma((n_row,)),
                dma((reductions, n_row)), dma((reductions, n_row)),
                dma((reductions, n_col)), dma((reductions, n_col)),
                dma((n_row,)), dma((n_row,)),
                dma((n_col,)), dma((n_col,)), dma((4,)),
            ],
            compiler_params=pltpu.CompilerParams(collective_id=0, has_side_effects=True),
        )(tiles, block_rows[0], block_cols[0], counts, seeds)

    return jax.shard_map(
        on_device,
        mesh=mesh,
        in_specs=(
            P("row", "col", None, None, None),
            P("row", "col", None),
            P("row", "col", None),
            P("row", "col"),
            P(None, ("col", "row")),
        ),
        out_specs=(P(None, ("col", "row")), P()),
        check_vma=False,
    )
```

```python
import functools

import jax
import jax.numpy as jnp
from jax import lax
from jax.experimental import pallas as pl
from jax.experimental.pallas import tpu as pltpu
from jax.sharding import PartitionSpec as P

BLOCK = 128
ITERS = 4
ROW_CAP = 4
K = 8
UNROLL = 128
PARTS = 2
DEAD = 1024
F32 = jnp.float32
BF16 = jnp.bfloat16
I32 = jnp.int32


def within(index, most):
    return jnp.minimum(jnp.maximum(index, 0), most)


def ring(delta, size):
    return min(delta % size, -delta % size)


def split(value):
    high = value.astype(BF16)
    rest = value - high.astype(F32)
    middle = rest.astype(BF16)
    low = (rest - middle.astype(F32)).astype(BF16)
    return high, middle, low


def kernel(
    nx, ny, nz, pb, nodes,
    tiles_ref, rows_hbm, cols_hbm, counts_hbm, seeds_hbm,
    out_ref, deltas_ref,
    rows_ref, cols_ref, counts_ref, seeds_ref,
    a_buf, t_buf, g_even, g_odd, s_all, y_buf, p_buf, inc_even, inc_odd, v_buf, raw_buf, w_buf,
    p_deg, inc_deg, w_row, w_all, ut_buf, u_send, u_in, u_buf,
    tab_v, tab_s, rank_v, ctab_v, ctab_s, ar_a, ar_b, st_a, st_b,
    a_sem, tab_sem, gr_sem, gs_sem, er_sem, es_sem, cr_sem, cs_sem, ra_sem, sa_sem, rb_sem, sb_sem,
    wr_sem, ws_sem, ur_sem, us_sem, in_sem,
):
    n_row, n_col = nx * ny, nz * 2
    g_buf, inc_buf = (g_even, g_odd, s_all), (inc_even, inc_odd)
    tile_total = a_buf.shape[0]
    slots = n_row * ROW_CAP
    row_blocks, col_blocks = n_row * pb, n_col * pb
    i = lax.axis_index("row")
    j = lax.axis_index("col")
    px, py = i // ny, i % ny
    z, c = j // 2, j % 2
    other = z * 2 + (1 - c)

    row_offsets = sorted(
        [(dx, dy) for dx in range(nx) for dy in range(ny) if (dx, dy) != (0, 0)],
        key=lambda d: -(ring(d[0], nx) + ring(d[1], ny)),
    )

    def row_peer(d):
        return lax.rem(px + d[0], nx) * ny + lax.rem(py + d[1], ny)

    def row_index(d):
        return d[0] * ny + d[1]

    def col_of(dz):
        return lax.rem(z + dz, nz) * 2 + c

    small = [
        pltpu.make_async_copy(source, target, in_sem.at[k])
        for k, (source, target) in enumerate(
            [
                (seeds_hbm, seeds_ref),
                (rows_hbm, rows_ref),
                (cols_hbm, cols_ref),
                (counts_hbm, counts_ref),
            ]
        )
    ]
    for copy in small:
        copy.start()
    barrier = pltpu.get_barrier_semaphore()
    for d in row_offsets:
        pl.semaphore_signal(barrier, inc=1, device_id={"row": row_peer(d)})
    for o in range(1, n_col):
        pl.semaphore_signal(barrier, inc=1, device_id={"col": lax.rem(j + o, n_col)})
    load = pltpu.make_async_copy(tiles_ref.at[0, 0], a_buf, a_sem)
    load.start()

    def exchange_copy(par, d):
        o = row_peer(d)
        there, here = pl.ds(o * ROW_CAP, ROW_CAP), pl.ds(i * ROW_CAP, ROW_CAP)
        sem = 2 if par is None else par
        return pltpu.make_async_remote_copy(
            src_ref=p_deg.at[there] if par is None else p_buf.at[par, there],
            dst_ref=inc_deg.at[here] if par is None else inc_buf[par].at[here],
            send_sem=es_sem.at[sem, row_index(d)],
            recv_sem=er_sem.at[sem, row_index(d)],
            device_id={"row": o},
        )

    def exchange_start(par):
        for d in row_offsets:
            exchange_copy(par, d).start()
        here = pl.ds(i * ROW_CAP, ROW_CAP)
        if par is None:
            inc_deg[here] = p_deg[here]
        else:
            inc_buf[par][here] = p_buf[par, here]

    def exchange_wait(par):
        for d in reversed(row_offsets):
            exchange_copy(par, d).wait_recv()

    def exchange_done(par):
        for d in row_offsets:
            exchange_copy(par, d).wait_send()

    def rank_copy(d):
        o = row_peer(d)
        return pltpu.make_async_remote_copy(
            src_ref=rank_v.at[o // per_half],
            dst_ref=ctab_v.at[i],
            send_sem=cs_sem.at[row_index(d)],
            recv_sem=cr_sem.at[row_index(d)],
            device_id={"row": o},
        )

    def weight_copy(d):
        return pltpu.make_async_remote_copy(
            src_ref=w_row,
            dst_ref=w_all.at[pl.ds(i * pb, pb)],
            send_sem=ws_sem.at[row_index(d)],
            recv_sem=wr_sem.at[row_index(d)],
            device_id={"row": row_peer(d)},
        )

    def u_copy(o):
        dest = lax.rem(j + o, n_col)
        return pltpu.make_async_remote_copy(
            src_ref=u_send.at[pl.ds(dest * pb, pb)],
            dst_ref=u_in.at[j],
            send_sem=us_sem.at[o],
            recv_sem=ur_sem.at[o],
            device_id={"col": dest},
        )

    cut = pb // PARTS

    def gather_copy(par, source, dest, sem, part):
        piece = g_buf[par].at[pl.ds(source * pb + part * cut, cut)]
        return pltpu.make_async_remote_copy(
            src_ref=piece,
            dst_ref=piece,
            send_sem=gs_sem.at[par, sem, part],
            recv_sem=gr_sem.at[par, source, part],
            device_id={"col": dest},
        )

    two_phase = nz == 8
    direct = [nz - 2, 2, nz - 1, 1] if two_phase else list(range(1, nz))
    sends = 15 if two_phase else 2 * nz - 1
    far = 2 + 4 * (1 - c)

    def arrived(par, source, part):
        gather_copy(par, source, other, 0, part).wait_recv()

    def gather_start(par, part):
        for k in range(len(direct)):
            gather_copy(par, j, col_of(direct[k]), k, part).start()
        gather_copy(par, j, other, len(direct), part).start()

    def gather_middle(par):
        if two_phase:
            for part in range(PARTS):
                arrived(par, col_of(6), part)
                gather_copy(par, col_of(6), col_of(1), 5, part).start()
                arrived(par, col_of(2), part)
                gather_copy(par, col_of(2), col_of(7), 6, part).start()
                gather_copy(par, col_of(8 - far), col_of(far), 7, part).start()
                gather_copy(par, col_of(6), other, 8, part).start()
                gather_copy(par, col_of(2), other, 9, part).start()

    def gather_wait(par, meanwhile=None):
        rest = [1, 7, 3, 5, 4] if two_phase else direct
        for first in range(0, len(rest), 2):
            for part in range(PARTS):
                for k in range(first, min(first + 2, len(rest))):
                    arrived(par, col_of(rest[k]), part)
                    gather_copy(
                        par, col_of(rest[k]), other, sends - len(rest) + k, part
                    ).start()
        if meanwhile is not None:
            meanwhile()
        for dz in [0, 1, nz - 1, 2, nz - 2, 3, nz - 3, 4] if two_phase else range(nz):
            for part in range(PARTS):
                arrived(par, lax.rem(z + dz, nz) * 2 + (1 - c), part)

    def gather_done(par):
        for sem in range(sends):
            for part in range(PARTS):
                gather_copy(par, j, other, sem, part).wait_send()

    def ar_row(n, d):
        return pltpu.make_async_remote_copy(
            src_ref=st_a.at[n], dst_ref=ar_a.at[n, i],
            send_sem=sa_sem.at[n, row_index(d)], recv_sem=ra_sem.at[n, row_index(d)],
            device_id={"row": row_peer(d)},
        )

    def ar_col(n, o):
        return pltpu.make_async_remote_copy(
            src_ref=st_b.at[n], dst_ref=ar_b.at[n, j],
            send_sem=sb_sem.at[n, o], recv_sem=rb_sem.at[n, o],
            device_id={"col": lax.rem(j + o, n_col)},
        )

    def tree(op, parts):
        while len(parts) > 1:
            parts = [functools.reduce(op, parts[k : k + 2]) for k in range(0, len(parts), 2)]
        return parts[0]

    def ar_start(n, value):
        st_a[n] = value
        ar_a[n, i] = value
        for d in row_offsets:
            ar_row(n, d).start()

    def ar_middle(n, op):
        for d in reversed(row_offsets):
            ar_row(n, d).wait_recv()
        value = tree(op, [ar_a[n, s] for s in range(n_row)])
        st_b[n] = value
        ar_b[n, j] = value
        for o in range(1, n_col):
            ar_col(n, o).start()

    def ar_end(n, op):
        for o in range(1, n_col):
            ar_col(n, o).wait_recv()
        value = tree(op, [ar_b[n, s] for s in range(n_col)])
        for d in row_offsets:
            ar_row(n, d).wait_send()
        for o in range(1, n_col):
            ar_col(n, o).wait_send()
        return value

    def scale_of(total):
        return nodes / jnp.broadcast_to(jnp.sum(total, axis=1, keepdims=True), (K, BLOCK))

    y_buf[tile_total] = jnp.zeros((K, BLOCK), F32)
    for par in range(2):
        inc_buf[par][slots] = jnp.zeros((K, BLOCK), F32)
    w_all[row_blocks] = jnp.zeros((1, BLOCK), F32)
    inc_deg[slots] = jnp.zeros((1, BLOCK), F32)
    small[0].wait()
    seed_sum = jnp.zeros((K, BLOCK), F32)
    for b in range(pb):
        seed = seeds_ref[:, b * BLOCK : (b + 1) * BLOCK].astype(F32)
        seed_sum += seed
        s_all[j * pb + b] = seeds_ref[:, b * BLOCK : (b + 1) * BLOCK].astype(jnp.int16)

    pl.semaphore_wait(barrier, n_row + n_col - 2)
    for part in range(PARTS):
        gather_start(2, part)
    ar_start(0, seed_sum)
    for copy in small[1:]:
        copy.wait()

    sub = lax.broadcasted_iota(I32, (tile_total, 128), 0)
    lane = lax.broadcasted_iota(I32, (tile_total, 128), 1)
    count = counts_ref[...]
    lane_row = lax.broadcasted_iota(I32, (1, 128), 1)
    key_r = jnp.where(lane_row < count, rows_ref[...], DEAD)
    key_rr = jnp.broadcast_to(key_r, (tile_total, 128))
    cols_rr = jnp.broadcast_to(cols_ref[...], (tile_total, 128))

    def lanes(value):
        return jnp.sum(value, axis=1, keepdims=True)

    def subs(value):
        return jnp.sum(value, axis=0, keepdims=True)

    def pick_if(mask, value):
        return jnp.where(mask, value, 0)

    key_c = lanes(pick_if(sub == lane, key_rr))
    cols_c = lanes(pick_if(sub == lane, cols_rr))
    key_cc = jnp.broadcast_to(key_c, (tile_total, 128))
    same = key_rr == key_cc
    before = lanes(pick_if(same & (lane < sub), 1))
    pos_c = before + lanes(pick_if(key_rr < key_cc, 1))
    last_c = lanes(pick_if(key_rr <= key_cc, 1)) - 1
    first_c = pick_if((before == 0) & (key_c < DEAD), 1)
    before_r = subs(pick_if(same & (sub < lane), 1))
    first_r = pick_if((before_r == 0) & (key_r < DEAD), 1)
    shift = pb.bit_length() - 1
    owner_c = key_c >> shift
    owner_r = key_r >> shift
    rank_c = lanes(
        pick_if((owner_r == owner_c) & (key_rr < key_cc), jnp.broadcast_to(first_r, sub.shape))
    )
    order = pos_c == lane
    slot_c = owner_c * ROW_CAP + rank_c
    chosen = slot_c == lane
    tab_v[0] = subs(pick_if(order, sub))
    tab_v[1] = subs(pick_if(order, cols_c))
    tab_v[2] = subs(pick_if(order, 1 - first_c))
    tab_v[3] = (
        subs(pick_if(chosen, first_c * last_c)) + (1 - subs(pick_if(chosen, first_c))) * tile_total
    )
    tab_v[4] = jnp.where(lane_row < count, rows_ref[...], row_blocks)
    tab_v[5] = jnp.where(
        subs(pick_if(chosen, first_c)) > 0, subs(pick_if(chosen, first_c * key_c)), row_blocks
    )
    per_half = 128 // pb
    for h in range(rank_v.shape[0]):
        found = subs(pick_if(key_c == lane + 128 * h, first_c * (rank_c + 1)))
        rank_v[h] = jnp.where(found > 0, found - 1 + i * ROW_CAP, slots)
    table = pltpu.make_async_copy(tab_v, tab_s, tab_sem)
    table.start()
    for d in row_offsets:
        rank_copy(d).start()
    table.wait()
    load.wait()
    ctab_v[i] = rank_v[i // per_half]

    def products(par, ones):
        def step(at, acc):
            for u in range(UNROLL):
                t = at * UNROLL + u
                if ones:
                    x = jnp.ones((K, BLOCK), BF16)
                    tile = a_buf[within(tab_s[0, 0, t], tile_total - 1)].T
                    t_buf[t] = tile
                else:
                    x = g_buf[par][within(tab_s[1, 0, t], col_blocks - 1)]
                    tile = t_buf[t]
                y = jnp.dot(x, tile, preferred_element_type=F32)
                acc = acc * tab_s[2, 0, t].astype(F32) + y
                y_buf[t] = acc
            return acc

        lax.fori_loop(0, tile_total // UNROLL, step, jnp.zeros((K, BLOCK), F32))

        for q in range(slots):
            value = y_buf[within(tab_s[3, 0, q], tile_total)]
            if ones:
                p_deg[q] = value[0:1]
            else:
                p_buf[par, q] = value

    def received(par, b):
        at = lax.rem(i, per_half) * pb + b
        source = inc_deg if par is None else inc_buf[par]
        return tree(
            jnp.add, [source[within(ctab_s[s, 0, at], slots)] for s in range(n_row)]
        )

    def transposed_products():
        sub8 = lax.broadcasted_iota(I32, (K, BLOCK), 0)

        def step(at, carry):
            for u in range(UNROLL):
                t = at * UNROLL + u
                w = w_all[within(tab_s[4, 0, t], row_blocks)]
                high, middle, low = (part.astype(F32) for part in split(w))
                rows = jnp.where(sub8 == 0, high, jnp.where(sub8 == 1, middle, low))
                rows = jnp.where(sub8 < 3, rows, 0.0).astype(BF16)
                y = jnp.dot(rows, a_buf[t], preferred_element_type=F32)
                ut_buf[pl.ds(t, 1), :] = jnp.sum(y, axis=0, keepdims=True)
            return carry

        lax.fori_loop(0, tile_total // UNROLL, step, 0)
        block_id = lax.broadcasted_iota(I32, (col_blocks, 128), 0)
        hot = jnp.where(block_id == cols_ref[...], 1.0, 0.0).astype(BF16)
        u_send[...] = sum(
            jnp.dot(hot, part, preferred_element_type=F32) for part in split(ut_buf[...])
        )

    def weighted(base):
        sums = [base] + [jnp.zeros((K, BLOCK), F32) for _ in range(3)]
        for q in range(slots):
            w = w_all[within(tab_s[5, 0, q], row_blocks)]
            sums[q % 4] += p_buf[0, q] * w
        return tree(jnp.add, sums)

    products(None, True)
    exchange_start(None)
    gather_middle(2)
    ar_middle(0, jnp.add)
    for d in row_offsets:
        rank_copy(d).wait_recv()
    ctable = pltpu.make_async_copy(ctab_v, ctab_s, tab_sem)
    ctable.start()
    exchange_wait(None)
    ctable.wait()

    for b in range(pb):
        w = 1.0 / (received(None, b) + 1.0)
        w_buf[b] = jnp.broadcast_to(w, (K, BLOCK))
        w_row[b] = w
    for d in row_offsets:
        weight_copy(d).start()
    w_all[pl.ds(i * pb, pb)] = w_row[...]
    gather_wait(2)
    seed_scale = scale_of(ar_end(0, jnp.add))

    def first_half(at, carry):
        for u in range(8):
            g_even[at * 8 + u] = (s_all[at * 8 + u].astype(I32).astype(F32) * seed_scale).astype(BF16)
        return carry

    lax.fori_loop(0, col_blocks // 8, first_half, 0)
    own_total = jnp.zeros((K, BLOCK), F32)
    for b in range(pb):
        v = seeds_ref[:, b * BLOCK : (b + 1) * BLOCK].astype(F32) * seed_scale
        v_buf[b] = v
        own_total += v * w_buf[b]
    products(0, False)
    for d in reversed(row_offsets):
        weight_copy(d).wait_recv()
    ar_start(1, weighted(own_total))
    exchange_start(0)
    transposed_products()
    for o in range(1, n_col):
        u_copy(o).start()
    u_in[j] = u_send[pl.ds(j * pb, pb)]
    ar_middle(1, jnp.add)
    gather_done(2)
    exchange_done(None)
    for d in row_offsets:
        rank_copy(d).wait_send()
    for o in range(1, n_col):
        u_copy(o).wait_recv()
    u_sum = tree(jnp.add, [u_in[s] for s in range(n_col)])
    for b in range(pb):
        u_buf[b] = u_sum[b : b + 1]

    changes = []
    for it in range(ITERS):
        par = it % 2
        if it > 0:
            gather_middle(par)
            gather_wait(par, functools.partial(ar_middle, it + 1, jnp.add))
            products(par, False)
            exchange_start(par)
            gather_done(par)
        if it == 0:
            exchange_wait(par)
        factor = scale_of(ar_end(it + 1, jnp.add))
        if it > 0:
            exchange_wait(par)

        for b in range(pb):
            v = (received(par, b) + v_buf[b]) * w_buf[b] * factor
            raw_buf[b] = v
            if it < ITERS - 1:
                g_buf[1 - par][j * pb + b] = v.astype(BF16)
                if (b + 1) % cut == 0:
                    gather_start(1 - par, b // cut)
        change = jnp.zeros((K, BLOCK), F32)
        total = jnp.zeros((K, BLOCK), F32)
        for b in range(pb):
            v = raw_buf[b]
            change = jnp.maximum(change, jnp.abs(v - v_buf[b]))
            if it < ITERS - 1:
                v_buf[b] = v
                total += v.astype(BF16).astype(F32) * u_buf[b] + v * w_buf[b]
        if it < ITERS - 1:
            ar_start(it + 2, total)
        exchange_done(par)
        if it == 0:
            for d in row_offsets:
                weight_copy(d).wait_send()
            for o in range(1, n_col):
                u_copy(o).wait_send()
        changes.append(jnp.max(change, axis=1, keepdims=True))

    sub8 = lax.broadcasted_iota(I32, (K, BLOCK), 0)
    lane8 = lax.broadcasted_iota(I32, (K, BLOCK), 1)
    packed = jnp.zeros((K, BLOCK), F32)
    for it in range(ITERS):
        as_row = jnp.sum(jnp.where(sub8 == lane8, changes[it], 0.0), axis=0, keepdims=True)
        packed = jnp.where(sub8 == it, as_row, packed)
    last = ITERS + 1
    ar_start(last, packed)
    for b in range(pb):
        out_ref[:, b * BLOCK : (b + 1) * BLOCK] = raw_buf[b]
    ar_middle(last, jnp.maximum)
    most = ar_end(last, jnp.maximum)
    deltas_ref[...] = most[0:ITERS, 0:K]


def solution(mesh, shape=(4, 4, 8)):
    nx, ny, nz = shape

    def on_device(tiles, block_rows, block_cols, counts, seeds):
        n_row, n_col = nx * ny, nz * 2
        tile_total = tiles.shape[2]
        piece = seeds.shape[1]
        pb = piece // BLOCK
        slots = n_row * ROW_CAP
        halves = max(1, n_row * pb // 128)
        nodes = float(piece * n_row * n_col)
        dma = pltpu.SemaphoreType.DMA
        reductions = ITERS + 2
        body = functools.partial(kernel, nx, ny, nz, pb, nodes)
        vmem = pl.BlockSpec(memory_space=pltpu.VMEM)
        return pl.pallas_call(
            body,
            out_shape=(
                pltpu.VMEM((K, piece), F32),
                pltpu.VMEM((ITERS, K), F32),
            ),
            in_specs=[
                pl.BlockSpec(memory_space=pltpu.HBM) for _ in range(5)
            ],
            out_specs=(vmem, vmem),
            scratch_shapes=[
                pltpu.VMEM((1, tile_total), I32),
                pltpu.VMEM((1, tile_total), I32),
                pltpu.VMEM((1, 1), I32),
                pltpu.VMEM((K, piece), I32),
                pltpu.VMEM((tile_total, BLOCK, BLOCK), BF16),
                pltpu.VMEM((tile_total, BLOCK, BLOCK), BF16),
                pltpu.VMEM((n_col * pb, K, BLOCK), BF16),
                pltpu.VMEM((n_col * pb, K, BLOCK), BF16),
                pltpu.VMEM((n_col * pb, K, BLOCK), jnp.int16),
                pltpu.VMEM((tile_total + 1, K, BLOCK), F32),
                pltpu.VMEM((2, slots, K, BLOCK), F32),
                pltpu.VMEM((slots + 1, K, BLOCK), F32),
                pltpu.VMEM((slots + 1, K, BLOCK), F32),
                pltpu.VMEM((pb, K, BLOCK), F32),
                pltpu.VMEM((pb, K, BLOCK), F32),
                pltpu.VMEM((pb, K, BLOCK), F32),
                pltpu.VMEM((slots, 1, BLOCK), F32),
                pltpu.VMEM((slots + 1, 1, BLOCK), F32),
                pltpu.VMEM((pb, 1, BLOCK), F32),
                pltpu.VMEM((n_row * pb + 1, 1, BLOCK), F32),
                pltpu.VMEM((tile_total, BLOCK), F32),
                pltpu.VMEM((n_col * pb, BLOCK), F32),
                pltpu.VMEM((n_col, pb, BLOCK), F32),
                pltpu.VMEM((pb, 1, BLOCK), F32),
                pltpu.VMEM((6, 1, 128), I32),
                pltpu.SMEM((6, 1, 128), I32),
                pltpu.VMEM((halves, 1, 128), I32),
                pltpu.VMEM((n_row, 1, 128), I32),
                pltpu.SMEM((n_row, 1, 128), I32),
                pltpu.VMEM((reductions, n_row, K, BLOCK), F32),
                pltpu.VMEM((reductions, n_col, K, BLOCK), F32),
                pltpu.VMEM((reductions, K, BLOCK), F32),
                pltpu.VMEM((reductions, K, BLOCK), F32),
                dma, dma,
                dma((3, n_col, PARTS)), dma((3, 2 * nz, PARTS)),
                dma((3, n_row)), dma((3, n_row)),
                dma((n_row,)), dma((n_row,)),
                dma((reductions, n_row)), dma((reductions, n_row)),
                dma((reductions, n_col)), dma((reductions, n_col)),
                dma((n_row,)), dma((n_row,)),
                dma((n_col,)), dma((n_col,)), dma((4,)),
            ],
            compiler_params=pltpu.CompilerParams(collective_id=0, has_side_effects=True),
        )(tiles, block_rows[0], block_cols[0], counts, seeds)

    return jax.shard_map(
        on_device,
        mesh=mesh,
        in_specs=(
            P("row", "col", None, None, None),
            P("row", "col", None),
            P("row", "col", None),
            P("row", "col"),
            P(None, ("col", "row")),
        ),
        out_specs=(P(None, ("col", "row")), P()),
        check_vma=False,
    )
```

```python
import functools

import jax
import jax.numpy as jnp
from jax import lax
from jax.experimental import pallas as pl
from jax.experimental.pallas import tpu as pltpu
from jax.sharding import PartitionSpec as P

BLOCK = 128
ITERS = 4
ROW_CAP = 4
K = 8
UNROLL = 128
PARTS = 2
DEAD = 1024
F32 = jnp.float32
BF16 = jnp.bfloat16
I32 = jnp.int32


def within(index, most):
    return jnp.minimum(jnp.maximum(index, 0), most)


def ring(delta, size):
    return min(delta % size, -delta % size)


def split(value):
    high = value.astype(BF16)
    rest = value - high.astype(F32)
    middle = rest.astype(BF16)
    low = (rest - middle.astype(F32)).astype(BF16)
    return high, middle, low


def kernel(
    nx, ny, nz, pb, nodes,
    tiles_ref, rows_hbm, cols_hbm, counts_hbm, seeds_hbm,
    out_ref, deltas_ref,
    rows_ref, cols_ref, counts_ref, seeds_ref,
    a_buf, t_buf, g_even, g_odd, s_all, y_buf, p_buf, inc_even, inc_odd, v_buf, raw_buf, w_buf,
    p_deg, inc_deg, w_row, w_all, ut_buf, u_send, u_in, u_buf,
    tab_v, tab_s, rank_v, ctab_v, ctab_s, ar_a, ar_b, st_a, st_b,
    a_sem, tab_sem, gr_sem, gs_sem, er_sem, es_sem, cr_sem, cs_sem, ra_sem, sa_sem, rb_sem, sb_sem,
    wr_sem, ws_sem, ur_sem, us_sem, in_sem,
):
    n_row, n_col = nx * ny, nz * 2
    g_buf, inc_buf = (g_even, g_odd, s_all), (inc_even, inc_odd)
    tile_total = a_buf.shape[0]
    slots = n_row * ROW_CAP
    row_blocks, col_blocks = n_row * pb, n_col * pb
    i = lax.axis_index("row")
    j = lax.axis_index("col")
    px, py = i // ny, i % ny
    z, c = j // 2, j % 2
    other = z * 2 + (1 - c)

    row_offsets = sorted(
        [(dx, dy) for dx in range(nx) for dy in range(ny) if (dx, dy) != (0, 0)],
        key=lambda d: -(ring(d[0], nx) + ring(d[1], ny)),
    )

    def row_peer(d):
        return lax.rem(px + d[0], nx) * ny + lax.rem(py + d[1], ny)

    def row_index(d):
        return d[0] * ny + d[1]

    def col_of(dz):
        return lax.rem(z + dz, nz) * 2 + c

    small = [
        pltpu.make_async_copy(source, target, in_sem.at[k])
        for k, (source, target) in enumerate(
            [
                (seeds_hbm, seeds_ref),
                (rows_hbm, rows_ref),
                (cols_hbm, cols_ref),
                (counts_hbm, counts_ref),
            ]
        )
    ]
    for copy in small:
        copy.start()
    barrier = pltpu.get_barrier_semaphore()
    for d in row_offsets:
        pl.semaphore_signal(barrier, inc=1, device_id={"row": row_peer(d)})
    for o in range(1, n_col):
        pl.semaphore_signal(barrier, inc=1, device_id={"col": lax.rem(j + o, n_col)})
    load = pltpu.make_async_copy(tiles_ref.at[0, 0], a_buf, a_sem)
    load.start()

    def exchange_copy(par, d):
        o = row_peer(d)
        there, here = pl.ds(o * ROW_CAP, ROW_CAP), pl.ds(i * ROW_CAP, ROW_CAP)
        sem = 2 if par is None else par
        return pltpu.make_async_remote_copy(
            src_ref=p_deg.at[there] if par is None else p_buf.at[par, there],
            dst_ref=inc_deg.at[here] if par is None else inc_buf[par].at[here],
            send_sem=es_sem.at[sem, row_index(d)],
            recv_sem=er_sem.at[sem, row_index(d)],
            device_id={"row": o},
        )

    def exchange_start(par):
        for d in row_offsets:
            exchange_copy(par, d).start()
        here = pl.ds(i * ROW_CAP, ROW_CAP)
        if par is None:
            inc_deg[here] = p_deg[here]
        else:
            inc_buf[par][here] = p_buf[par, here]

    def exchange_wait(par):
        for d in reversed(row_offsets):
            exchange_copy(par, d).wait_recv()

    def exchange_done(par):
        for d in row_offsets:
            exchange_copy(par, d).wait_send()

    def rank_copy(d):
        o = row_peer(d)
        return pltpu.make_async_remote_copy(
            src_ref=rank_v.at[o // per_half],
            dst_ref=ctab_v.at[i],
            send_sem=cs_sem.at[row_index(d)],
            recv_sem=cr_sem.at[row_index(d)],
            device_id={"row": o},
        )

    def weight_copy(d):
        return pltpu.make_async_remote_copy(
            src_ref=w_row,
            dst_ref=w_all.at[pl.ds(i * pb, pb)],
            send_sem=ws_sem.at[row_index(d)],
            recv_sem=wr_sem.at[row_index(d)],
            device_id={"row": row_peer(d)},
        )

    def u_copy(o):
        dest = lax.rem(j + o, n_col)
        return pltpu.make_async_remote_copy(
            src_ref=u_send.at[pl.ds(dest * pb, pb)],
            dst_ref=u_in.at[j],
            send_sem=us_sem.at[o],
            recv_sem=ur_sem.at[o],
            device_id={"col": dest},
        )

    cut = pb // PARTS

    def gather_copy(par, source, dest, sem, part):
        piece = g_buf[par].at[pl.ds(source * pb + part * cut, cut)]
        return pltpu.make_async_remote_copy(
            src_ref=piece,
            dst_ref=piece,
            send_sem=gs_sem.at[par, sem, part],
            recv_sem=gr_sem.at[par, source, part],
            device_id={"col": dest},
        )

    two_phase = nz == 8
    direct = [nz - 2, 2, nz - 1, 1] if two_phase else list(range(1, nz))
    sends = 15 if two_phase else 2 * nz - 1
    far = 2 + 4 * (1 - c)

    def arrived(par, source, part):
        gather_copy(par, source, other, 0, part).wait_recv()

    def gather_start(par, part):
        for k in range(len(direct)):
            gather_copy(par, j, col_of(direct[k]), k, part).start()
        gather_copy(par, j, other, len(direct), part).start()

    def gather_middle(par):
        if two_phase:
            for part in range(PARTS):
                arrived(par, col_of(6), part)
                gather_copy(par, col_of(6), col_of(1), 5, part).start()
                arrived(par, col_of(2), part)
                gather_copy(par, col_of(2), col_of(7), 6, part).start()
                gather_copy(par, col_of(8 - far), col_of(far), 7, part).start()
                gather_copy(par, col_of(6), other, 8, part).start()
                gather_copy(par, col_of(2), other, 9, part).start()

    def gather_wait(par, meanwhile=None):
        rest = [1, 7, 3, 5, 4] if two_phase else direct
        for first in range(0, len(rest), 2):
            for part in range(PARTS):
                for k in range(first, min(first + 2, len(rest))):
                    arrived(par, col_of(rest[k]), part)
                    gather_copy(
                        par, col_of(rest[k]), other, sends - len(rest) + k, part
                    ).start()
        if meanwhile is not None:
            meanwhile()
        for dz in [0, 1, nz - 1, 2, nz - 2, 3, nz - 3, 4] if two_phase else range(nz):
            for part in range(PARTS):
                arrived(par, lax.rem(z + dz, nz) * 2 + (1 - c), part)

    def gather_done(par):
        for sem in range(sends):
            for part in range(PARTS):
                gather_copy(par, j, other, sem, part).wait_send()

    def ar_row(n, d):
        return pltpu.make_async_remote_copy(
            src_ref=st_a.at[n], dst_ref=ar_a.at[n, i],
            send_sem=sa_sem.at[n, row_index(d)], recv_sem=ra_sem.at[n, row_index(d)],
            device_id={"row": row_peer(d)},
        )

    def ar_col(n, o):
        return pltpu.make_async_remote_copy(
            src_ref=st_b.at[n], dst_ref=ar_b.at[n, j],
            send_sem=sb_sem.at[n, o], recv_sem=rb_sem.at[n, o],
            device_id={"col": lax.rem(j + o, n_col)},
        )

    def tree(op, parts):
        while len(parts) > 1:
            parts = [functools.reduce(op, parts[k : k + 2]) for k in range(0, len(parts), 2)]
        return parts[0]

    def ar_start(n, value):
        st_a[n] = value
        ar_a[n, i] = value
        for d in row_offsets:
            ar_row(n, d).start()

    def ar_middle(n, op):
        for d in reversed(row_offsets):
            ar_row(n, d).wait_recv()
        value = tree(op, [ar_a[n, s] for s in range(n_row)])
        st_b[n] = value
        ar_b[n, j] = value
        for o in range(1, n_col):
            ar_col(n, o).start()

    def ar_end(n, op):
        for o in range(1, n_col):
            ar_col(n, o).wait_recv()
        value = tree(op, [ar_b[n, s] for s in range(n_col)])
        for d in row_offsets:
            ar_row(n, d).wait_send()
        for o in range(1, n_col):
            ar_col(n, o).wait_send()
        return value

    def scale_of(total):
        return nodes / jnp.broadcast_to(jnp.sum(total, axis=1, keepdims=True), (K, BLOCK))

    y_buf[tile_total] = jnp.zeros((K, BLOCK), F32)
    for par in range(2):
        inc_buf[par][slots] = jnp.zeros((K, BLOCK), F32)
    w_all[row_blocks] = jnp.zeros((1, BLOCK), F32)
    inc_deg[slots] = jnp.zeros((1, BLOCK), F32)
    small[0].wait()
    seed_sum = jnp.zeros((K, BLOCK), F32)
    for b in range(pb):
        seed = seeds_ref[:, b * BLOCK : (b + 1) * BLOCK].astype(F32)
        seed_sum += seed
        s_all[j * pb + b] = seeds_ref[:, b * BLOCK : (b + 1) * BLOCK].astype(jnp.int16)

    pl.semaphore_wait(barrier, n_row + n_col - 2)
    for part in range(PARTS):
        gather_start(2, part)
    ar_start(0, seed_sum)
    for copy in small[1:]:
        copy.wait()

    sub = lax.broadcasted_iota(I32, (tile_total, 128), 0)
    lane = lax.broadcasted_iota(I32, (tile_total, 128), 1)
    count = counts_ref[...]
    lane_row = lax.broadcasted_iota(I32, (1, 128), 1)
    key_r = jnp.where(lane_row < count, rows_ref[...], DEAD)
    key_rr = jnp.broadcast_to(key_r, (tile_total, 128))
    cols_rr = jnp.broadcast_to(cols_ref[...], (tile_total, 128))

    def lanes(value):
        return jnp.sum(value, axis=1, keepdims=True)

    def subs(value):
        return jnp.sum(value, axis=0, keepdims=True)

    def pick_if(mask, value):
        return jnp.where(mask, value, 0)

    key_c = lanes(pick_if(sub == lane, key_rr))
    cols_c = lanes(pick_if(sub == lane, cols_rr))
    key_cc = jnp.broadcast_to(key_c, (tile_total, 128))
    same = key_rr == key_cc
    before = lanes(pick_if(same & (lane < sub), 1))
    pos_c = before + lanes(pick_if(key_rr < key_cc, 1))
    last_c = lanes(pick_if(key_rr <= key_cc, 1)) - 1
    first_c = pick_if((before == 0) & (key_c < DEAD), 1)
    before_r = subs(pick_if(same & (sub < lane), 1))
    first_r = pick_if((before_r == 0) & (key_r < DEAD), 1)
    shift = pb.bit_length() - 1
    owner_c = key_c >> shift
    owner_r = key_r >> shift
    rank_c = lanes(
        pick_if((owner_r == owner_c) & (key_rr < key_cc), jnp.broadcast_to(first_r, sub.shape))
    )
    order = pos_c == lane
    slot_c = owner_c * ROW_CAP + rank_c
    chosen = slot_c == lane
    tab_v[0] = subs(pick_if(order, sub))
    tab_v[1] = subs(pick_if(order, cols_c))
    tab_v[2] = subs(pick_if(order, 1 - first_c))
    tab_v[3] = (
        subs(pick_if(chosen, first_c * last_c)) + (1 - subs(pick_if(chosen, first_c))) * tile_total
    )
    tab_v[4] = jnp.where(lane_row < count, rows_ref[...], row_blocks)
    tab_v[5] = jnp.where(
        subs(pick_if(chosen, first_c)) > 0, subs(pick_if(chosen, first_c * key_c)), row_blocks
    )
    per_half = 128 // pb
    for h in range(rank_v.shape[0]):
        found = subs(pick_if(key_c == lane + 128 * h, first_c * (rank_c + 1)))
        rank_v[h] = jnp.where(found > 0, found - 1 + i * ROW_CAP, slots)
    table = pltpu.make_async_copy(tab_v, tab_s, tab_sem)
    table.start()
    for d in row_offsets:
        rank_copy(d).start()
    table.wait()
    load.wait()
    ctab_v[i] = rank_v[i // per_half]

    def products(par, ones):
        def step(at, acc):
            for u in range(UNROLL):
                t = at * UNROLL + u
                if ones:
                    x = jnp.ones((K, BLOCK), BF16)
                    tile = a_buf[within(tab_s[0, 0, t], tile_total - 1)].T
                    t_buf[t] = tile
                else:
                    x = g_buf[par][within(tab_s[1, 0, t], col_blocks - 1)]
                    tile = t_buf[t]
                y = jnp.dot(x, tile, preferred_element_type=F32)
                acc = acc * tab_s[2, 0, t].astype(F32) + y
                y_buf[t] = acc
            return acc

        lax.fori_loop(0, tile_total // UNROLL, step, jnp.zeros((K, BLOCK), F32))

        for q in range(slots):
            value = y_buf[within(tab_s[3, 0, q], tile_total)]
            if ones:
                p_deg[q] = value[0:1]
            else:
                p_buf[par, q] = value

    def received(par, b):
        at = lax.rem(i, per_half) * pb + b
        source = inc_deg if par is None else inc_buf[par]
        return tree(
            jnp.add, [source[within(ctab_s[s, 0, at], slots)] for s in range(n_row)]
        )

    def transposed_products():
        sub8 = lax.broadcasted_iota(I32, (K, BLOCK), 0)

        def step(at, carry):
            for u in range(UNROLL):
                t = at * UNROLL + u
                w = w_all[within(tab_s[4, 0, t], row_blocks)]
                high, middle, low = (part.astype(F32) for part in split(w))
                rows = jnp.where(sub8 == 0, high, jnp.where(sub8 == 1, middle, low))
                rows = jnp.where(sub8 < 3, rows, 0.0).astype(BF16)
                y = jnp.dot(rows, a_buf[t], preferred_element_type=F32)
                ut_buf[pl.ds(t, 1), :] = jnp.sum(y, axis=0, keepdims=True)
            return carry

        lax.fori_loop(0, tile_total // UNROLL, step, 0)
        block_id = lax.broadcasted_iota(I32, (col_blocks, 128), 0)
        hot = jnp.where(block_id == cols_ref[...], 1.0, 0.0).astype(BF16)
        u_send[...] = sum(
            jnp.dot(hot, part, preferred_element_type=F32) for part in split(ut_buf[...])
        )

    def weighted(base):
        sums = [base] + [jnp.zeros((K, BLOCK), F32) for _ in range(3)]
        for q in range(slots):
            w = w_all[within(tab_s[5, 0, q], row_blocks)]
            sums[q % 4] += p_buf[0, q] * w
        return tree(jnp.add, sums)

    products(None, True)
    exchange_start(None)
    gather_middle(2)
    ar_middle(0, jnp.add)
    for d in row_offsets:
        rank_copy(d).wait_recv()
    ctable = pltpu.make_async_copy(ctab_v, ctab_s, tab_sem)
    ctable.start()
    exchange_wait(None)
    ctable.wait()

    for b in range(pb):
        w = 1.0 / (received(None, b) + 1.0)
        w_buf[b] = jnp.broadcast_to(w, (K, BLOCK))
        w_row[b] = w
    for d in row_offsets:
        weight_copy(d).start()
    w_all[pl.ds(i * pb, pb)] = w_row[...]
    own_total = jnp.zeros((K, BLOCK), F32)
    for b in range(pb):
        own_total += seeds_ref[:, b * BLOCK : (b + 1) * BLOCK].astype(F32) * w_buf[b]
    gather_wait(2)
    seed_scale = scale_of(ar_end(0, jnp.add))

    def first_half(at, carry):
        for u in range(32):
            g_even[at * 32 + u] = (s_all[at * 32 + u].astype(I32).astype(F32) * seed_scale).astype(BF16)
        return carry

    lax.fori_loop(0, col_blocks // 32, first_half, 0)
    products(0, False)
    for d in reversed(row_offsets):
        weight_copy(d).wait_recv()
    ar_start(1, weighted(own_total * seed_scale))
    exchange_start(0)
    for b in range(pb):
        v_buf[b] = seeds_ref[:, b * BLOCK : (b + 1) * BLOCK].astype(F32) * seed_scale
    transposed_products()
    for o in range(1, n_col):
        u_copy(o).start()
    u_in[j] = u_send[pl.ds(j * pb, pb)]
    ar_middle(1, jnp.add)
    gather_done(2)
    exchange_done(None)
    for d in row_offsets:
        rank_copy(d).wait_send()
    for o in range(1, n_col):
        u_copy(o).wait_recv()
    u_sum = tree(jnp.add, [u_in[s] for s in range(n_col)])
    for b in range(pb):
        u_buf[b] = u_sum[b : b + 1]

    changes = []
    for it in range(ITERS):
        par = it % 2
        if it > 0:
            gather_middle(par)
            gather_wait(par, functools.partial(ar_middle, it + 1, jnp.add))
            products(par, False)
            exchange_start(par)
            gather_done(par)
        if it == 0:
            exchange_wait(par)
        factor = scale_of(ar_end(it + 1, jnp.add))
        if it > 0:
            exchange_wait(par)

        for b in range(pb):
            v = (received(par, b) + v_buf[b]) * w_buf[b] * factor
            raw_buf[b] = v
            if it < ITERS - 1:
                g_buf[1 - par][j * pb + b] = v.astype(BF16)
                if (b + 1) % cut == 0:
                    gather_start(1 - par, b // cut)
        change = jnp.zeros((K, BLOCK), F32)
        total = jnp.zeros((K, BLOCK), F32)
        for b in range(pb):
            v = raw_buf[b]
            change = jnp.maximum(change, jnp.abs(v - v_buf[b]))
            if it < ITERS - 1:
                v_buf[b] = v
                total += v.astype(BF16).astype(F32) * u_buf[b] + v * w_buf[b]
        if it < ITERS - 1:
            ar_start(it + 2, total)
        exchange_done(par)
        if it == 0:
            for d in row_offsets:
                weight_copy(d).wait_send()
            for o in range(1, n_col):
                u_copy(o).wait_send()
        changes.append(jnp.max(change, axis=1, keepdims=True))

    sub8 = lax.broadcasted_iota(I32, (K, BLOCK), 0)
    lane8 = lax.broadcasted_iota(I32, (K, BLOCK), 1)
    packed = jnp.zeros((K, BLOCK), F32)
    for it in range(ITERS):
        as_row = jnp.sum(jnp.where(sub8 == lane8, changes[it], 0.0), axis=0, keepdims=True)
        packed = jnp.where(sub8 == it, as_row, packed)
    last = ITERS + 1
    ar_start(last, packed)
    for b in range(pb):
        out_ref[:, b * BLOCK : (b + 1) * BLOCK] = raw_buf[b]
    ar_middle(last, jnp.maximum)
    most = ar_end(last, jnp.maximum)
    deltas_ref[...] = most[0:ITERS, 0:K]


def solution(mesh, shape=(4, 4, 8)):
    nx, ny, nz = shape

    def on_device(tiles, block_rows, block_cols, counts, seeds):
        n_row, n_col = nx * ny, nz * 2
        tile_total = tiles.shape[2]
        piece = seeds.shape[1]
        pb = piece // BLOCK
        slots = n_row * ROW_CAP
        halves = max(1, n_row * pb // 128)
        nodes = float(piece * n_row * n_col)
        dma = pltpu.SemaphoreType.DMA
        reductions = ITERS + 2
        body = functools.partial(kernel, nx, ny, nz, pb, nodes)
        vmem = pl.BlockSpec(memory_space=pltpu.VMEM)
        return pl.pallas_call(
            body,
            out_shape=(
                pltpu.VMEM((K, piece), F32),
                pltpu.VMEM((ITERS, K), F32),
            ),
            in_specs=[
                pl.BlockSpec(memory_space=pltpu.HBM) for _ in range(5)
            ],
            out_specs=(vmem, vmem),
            scratch_shapes=[
                pltpu.VMEM((1, tile_total), I32),
                pltpu.VMEM((1, tile_total), I32),
                pltpu.VMEM((1, 1), I32),
                pltpu.VMEM((K, piece), I32),
                pltpu.VMEM((tile_total, BLOCK, BLOCK), BF16),
                pltpu.VMEM((tile_total, BLOCK, BLOCK), BF16),
                pltpu.VMEM((n_col * pb, K, BLOCK), BF16),
                pltpu.VMEM((n_col * pb, K, BLOCK), BF16),
                pltpu.VMEM((n_col * pb, K, BLOCK), jnp.int16),
                pltpu.VMEM((tile_total + 1, K, BLOCK), F32),
                pltpu.VMEM((2, slots, K, BLOCK), F32),
                pltpu.VMEM((slots + 1, K, BLOCK), F32),
                pltpu.VMEM((slots + 1, K, BLOCK), F32),
                pltpu.VMEM((pb, K, BLOCK), F32),
                pltpu.VMEM((pb, K, BLOCK), F32),
                pltpu.VMEM((pb, K, BLOCK), F32),
                pltpu.VMEM((slots, 1, BLOCK), F32),
                pltpu.VMEM((slots + 1, 1, BLOCK), F32),
                pltpu.VMEM((pb, 1, BLOCK), F32),
                pltpu.VMEM((n_row * pb + 1, 1, BLOCK), F32),
                pltpu.VMEM((tile_total, BLOCK), F32),
                pltpu.VMEM((n_col * pb, BLOCK), F32),
                pltpu.VMEM((n_col, pb, BLOCK), F32),
                pltpu.VMEM((pb, 1, BLOCK), F32),
                pltpu.VMEM((6, 1, 128), I32),
                pltpu.SMEM((6, 1, 128), I32),
                pltpu.VMEM((halves, 1, 128), I32),
                pltpu.VMEM((n_row, 1, 128), I32),
                pltpu.SMEM((n_row, 1, 128), I32),
                pltpu.VMEM((reductions, n_row, K, BLOCK), F32),
                pltpu.VMEM((reductions, n_col, K, BLOCK), F32),
                pltpu.VMEM((reductions, K, BLOCK), F32),
                pltpu.VMEM((reductions, K, BLOCK), F32),
                dma, dma,
                dma((3, n_col, PARTS)), dma((3, 2 * nz, PARTS)),
                dma((3, n_row)), dma((3, n_row)),
                dma((n_row,)), dma((n_row,)),
                dma((reductions, n_row)), dma((reductions, n_row)),
                dma((reductions, n_col)), dma((reductions, n_col)),
                dma((n_row,)), dma((n_row,)),
                dma((n_col,)), dma((n_col,)), dma((4,)),
            ],
            compiler_params=pltpu.CompilerParams(collective_id=0, has_side_effects=True),
        )(tiles, block_rows[0], block_cols[0], counts, seeds)

    return jax.shard_map(
        on_device,
        mesh=mesh,
        in_specs=(
            P("row", "col", None, None, None),
            P("row", "col", None),
            P("row", "col", None),
            P("row", "col"),
            P(None, ("col", "row")),
        ),
        out_specs=(P(None, ("col", "row")), P()),
        check_vma=False,
    )
```
